32 devices in a mesh: gx: 4 (over y, x), gy: 2 (over core), gz: 4 (over z).
Axes of the slice: x: 2, y: 2, z: 4, core: 2. Of those that a mesh axis runs over, the one named last changes fastest.
Arguments:
- pair_blocks: float32 [529, 1024], P(None, ('gx', 'gy', 'gz')), may hold values from -6 to 6
- basis_map: float32 [529, 64], replicated, may hold values from -0.25 to 0.25
- pair_cells: int32 [3, 1024], P(None, ('gx', 'gy', 'gz')), may hold values from 0 to 511, as said below
- pair_offsets: float32 [3, 1024], P(None, ('gx', 'gy', 'gz')), may hold values from 0 to 1
- exponent_index: int32 [1024], P(('gx', 'gy', 'gz')), may hold values from 0 to 15
- radius_index: int32 [1024], P(('gx', 'gy', 'gz')), may hold values from 0 to 4
- exponents: float32 [16], replicated, may hold values from 7 to 9
Outputs:
- density: float32 [32, 64, 512], P('gx', 'gy', 'gz')
- spectrum: float32 [2, 512, 64, 32], P(None, ('gy', 'gz'), 'gx')
The draws below stay inside these ranges and needn't reach their ends.
Inputs may be any that keep to these rules, and one draw needn't show every extreme that they name: The y of pair_cells column p lies among the 32 cells, and its z among the 128 cells, of the gy and gz index of the device that holds column p. Of the pairs that one device holds at most 16 have x in the same run of 8 cells that one gx index holds, and in every draw some such run gets exactly 16 from every device.
All inputs are finite; a program needn't handle non-finite values.
Results may differ from the reference program's by a relative error of at most 0.0003.
Values sent between devices are 32-bit elements; how exact they have to be, the bound alone decides.
A program may use at most 64 MiB of HBM per device.

```python
import math
import jax
import jax.numpy as jnp
from jax import lax

BLOCK = 23
DEG = 3
NPOLY = 64
NEXP = 16
HALO = 8
CX = 8
CY = 32
CZ = 128
PAIR_DEV = 32
CAP = 16
PAIRS = 1024
NX = 32
NY = 64
NZ = 512
N_GX = 4
N_GY = 2
N_GZ = 4


def draw_pair_cells(key, part):
    source_count = N_GX * N_GY * N_GZ
    slot_count = N_GX * CAP
    key_level, key_top, key_pick, key_perm, key_x, key_y, key_z = jax.random.split(key, 7)
    levels = jax.random.randint(key_level, (N_GX,), 0, 4)
    favourite = jax.random.randint(key_top, (), 0, N_GX)
    levels = jnp.where(jnp.arange(N_GX) == favourite, 4, levels)
    sources = jnp.arange(source_count, dtype=jnp.int32)
    slot_ids = jnp.arange(slot_count, dtype=jnp.int32)
    slot_target = slot_ids // CAP
    first_slot = slot_ids % CAP == 0
    edge_class = (slot_target[None, :] + sources[:, None]) % 4
    upper_edge = first_slot[None, :] & (edge_class == 0)
    lower_edge = first_slot[None, :] & (edge_class == 2)
    slot_levels = jnp.where(upper_edge | lower_edge, 5, levels[slot_target][None, :])
    noise = jax.random.randint(key_pick, (source_count, slot_count), 0, 65536)
    scores = (slot_levels * 65536 + noise) * slot_count + slot_ids[None, :]
    unused, chosen = lax.top_k(scores, PAIR_DEV)
    orders = jax.vmap(lambda sub_key: jax.random.permutation(sub_key, PAIR_DEV))(jax.random.split(key_perm, source_count))
    chosen = jnp.take_along_axis(chosen, orders, 1)
    targets = chosen // CAP
    chosen_upper = jnp.take_along_axis(upper_edge, chosen, 1)
    chosen_lower = jnp.take_along_axis(lower_edge, chosen, 1)
    source_y = sources // N_GZ % N_GY
    source_z = sources % N_GZ
    inner_x = jax.random.randint(key_x, (source_count, PAIR_DEV), 0, CX)
    inner_x = jnp.where(chosen_upper, CX - 1, jnp.where(chosen_lower, 0, inner_x))
    cells_x = targets * CX + inner_x
    cells_y = source_y[:, None] * CY + jax.random.randint(key_y, (source_count, PAIR_DEV), 0, CY)
    cells_z = source_z[:, None] * CZ + jax.random.randint(key_z, (source_count, PAIR_DEV), 0, CZ)
    return jnp.stack([cells_x, cells_y, cells_z]).reshape(3, source_count * PAIR_DEV).astype(jnp.int32)


def set_ends(entries, own_key, low, high):
    extent = entries.shape
    place = [jax.random.randint(jax.random.fold_in(own_key, axis), (), 0, extent[axis]) for axis in range(len(extent))]
    entries = entries.at[tuple(place)].set(low)
    longest = extent.index(max(extent))
    place[longest] = (place[longest] + 1) % extent[longest]
    return entries.at[tuple(place)].set(high)


def steps_of(stream_key, dims, cuts, low, largest):
    level = 1.0
    for position, blocks in cuts:
        steps = jax.random.uniform(jax.random.fold_in(jax.random.fold_in(stream_key, 6), position), (blocks,), jnp.float32, low / len(cuts), largest / len(cuts))
        level = level * jnp.repeat(jnp.exp(steps), dims[position] // blocks).reshape((-1,) + (1,) * (len(dims) - 1 - position))
    return level


def centred(rng, dims, scale, limit, shards=(), kind=jnp.bfloat16):
    factor_of = steps_of(rng, dims, shards, -0.22, 0.18) if shards else 1.0
    entries = jax.random.normal(rng, dims, jnp.float32) * scale * factor_of
    return jnp.minimum(jnp.maximum(entries, -limit), limit).astype(kind)


def setup_inputs(seed: int = 0) -> dict:
    seeds = jax.random.split(jax.random.key(seed), 8)
    pair_blocks = centred(seeds[0], (BLOCK * BLOCK, PAIRS), 1.0, 6.0, ((1, 32),), jnp.float32)
    basis_map = centred(seeds[1], (BLOCK * BLOCK, NPOLY), (BLOCK * BLOCK) ** -0.5, 0.25, (), jnp.float32)
    pair_cells = draw_pair_cells(jax.random.fold_in(seeds[7], 71), 0)
    pair_offsets = jnp.clip(1.0 * jax.random.uniform(seeds[3], (3, PAIRS), jnp.float32) ** steps_of(seeds[3], (3, PAIRS), ((1, 32),), -0.2, 0.2), 0.0, 1.0)
    exponent_index = set_ends(jax.random.randint(seeds[4], (PAIRS,), 0, NEXP), jax.random.fold_in(seeds[4], 1), 0, NEXP - 1).astype(jnp.int32)
    radius_index = set_ends(jax.random.randint(seeds[5], (PAIRS,), 0, HALO // 2 + 1), jax.random.fold_in(seeds[5], 1), 0, (HALO // 2 + 1) - 1).astype(jnp.int32)
    exponents = jnp.clip(jnp.exp(jax.random.uniform(seeds[6], (NEXP,), jnp.float32, math.log(7.0), math.log(9.0))), 7.0, 9.0)
    return dict(pair_blocks=pair_blocks, basis_map=basis_map, pair_cells=pair_cells, pair_offsets=pair_offsets, exponent_index=exponent_index, radius_index=radius_index, exponents=exponents)


highest = lax.Precision.HIGHEST


def pair_factors(offsets_row, exponent_values, radius_cells):
    span = jnp.arange(2 * HALO + 1, dtype=jnp.int32) - HALO
    distance = span[None, :].astype(jnp.float32) - offsets_row[:, None]
    inside = (jnp.abs(span)[None, :] <= radius_cells[:, None]).astype(jnp.float32)
    envelope = jnp.exp(-exponent_values[:, None] * distance * distance) * inside
    scaled = distance / HALO
    return jnp.stack([scaled ** degree * envelope for degree in range(DEG + 1)], 1)


def reference(pair_blocks, basis_map, pair_cells, pair_offsets, exponent_index, radius_index, exponents):
    side = DEG + 1
    pair_total = pair_blocks.shape[1]
    group_size = 64
    group_count = pair_total // group_size
    coefficients = jnp.dot(basis_map.T, pair_blocks, precision=highest)
    radius_cells = HALO - radius_index
    radius_float = radius_cells.astype(jnp.float32)
    exponent_values = exponents[exponent_index] / (radius_float * radius_float)
    span = jnp.arange(2 * HALO + 1, dtype=jnp.int32) - HALO

    def regroup(values):
        return values.reshape((group_count, group_size) + values.shape[1:])

    pieces_all = (regroup(coefficients.T.reshape(pair_total, side, side, side)),
                  regroup(pair_factors(pair_offsets[0], exponent_values, radius_cells)),
                  regroup(pair_factors(pair_offsets[1], exponent_values, radius_cells)),
                  regroup(pair_factors(pair_offsets[2], exponent_values, radius_cells)),
                  regroup(pair_cells.T))

    def add_group(density_grid, pieces):
        pair_coefs, along_x, along_y, along_z, centre_cells = pieces
        partial_z = jnp.einsum('sijk,skc->sijc', pair_coefs, along_z, precision=highest)
        partial_y = jnp.einsum('sjb,sijc->sibc', along_y, partial_z, precision=highest)
        tile_values = jnp.einsum('sia,sibc->sabc', along_x, partial_y, precision=highest)
        rows_x = (centre_cells[:, 0:1] + span[None, :]) % NX
        rows_y = (centre_cells[:, 1:2] + span[None, :]) % NY
        rows_z = (centre_cells[:, 2:3] + span[None, :]) % NZ
        density_grid = density_grid.at[rows_x[:, :, None, None], rows_y[:, None, :, None], rows_z[:, None, None, :]].add(tile_values)
        return density_grid, None

    density, unused = lax.scan(add_group, jnp.zeros((NX, NY, NZ), jnp.float32), pieces_all)
    transform = jnp.fft.fftn(jnp.transpose(density, (2, 1, 0)), norm="ortho")
    spectrum = jnp.stack([jnp.real(transform), jnp.imag(transform)]).astype(jnp.float32)
    return density, spectrum
```

```python
import functools
import math

import jax
import jax.numpy as jnp
import ml_dtypes
import numpy as np
from jax import lax
from jax.experimental import pallas as pl
from jax.experimental.pallas import tpu as pltpu
from jax.sharding import PartitionSpec as P

DEG = 3
HALO = 8
CX = 8
CY = 32
CZ = 128
SIDE = DEG + 1
LANES = 128
SPAN = 32
VMEM_LIMIT = 40 << 20
COEFS = SIDE**3
FOLD = 4
TOP = COEFS // FOLD
BLOCK_ROWS = TOP + 8
CYW = CY + 2 * HALO
DEPTH = SIDE * LANES

f32 = jnp.float32
bf16 = jnp.bfloat16


def iota_f(shape, dim):
    return lax.broadcasted_iota(jnp.int32, shape, dim).astype(f32)


def cos_sin(turns):
    r = turns - jnp.floor(turns + 0.5)
    t = r * math.pi
    t2 = t * t
    s = t * _poly(t2, [(-1) ** n / math.factorial(2 * n + 1) for n in range(7)])
    c = _poly(t2, [(-1) ** n / math.factorial(2 * n) for n in range(8)])
    return 1.0 - 2.0 * s * s, 2.0 * s * c


def _poly(x, coefs):
    out = jnp.full_like(x, coefs[-1])
    for a in reversed(coefs[:-1]):
        out = out * x + a
    return out


def wrapped(cells, centre, total):
    d = cells - centre
    d = jnp.where(d < -HALO, d + total, d)
    return jnp.where(d > total - 1 - HALO, d - total, d)


def factors(offset, within, rate, radius):
    u = offset - within
    env = jnp.where(jnp.abs(offset) <= radius, jnp.exp(-rate * u * u), 0.0)
    s = u * (1.0 / HALO)
    out = [env]
    for _ in range(DEG):
        out.append(out[-1] * s)
    return out


def split(v):
    hi = v.astype(bf16)
    return hi, (v - hi.astype(f32)).astype(bf16)


def nt(a, b):
    return lax.dot_general(a, b, (((1,), (1,)), ((), ())), preferred_element_type=f32)


def span_part(within, rate, radius, table):
    offs = iota_f((SPAN, LANES), 0) - HALO
    four = jnp.concatenate(factors(offs, within, rate, radius), axis=1)
    hi, lo = split(four)
    return jnp.dot(table, jnp.concatenate([hi, lo, hi], axis=0), preferred_element_type=f32)


def span_table(frequency, length):
    offs = iota_f((1, SPAN), 1) - HALO
    c, s = cos_sin(frequency * offs * (1.0 / length))
    hi, lo = split(jnp.concatenate([c, -s], axis=0))
    return jnp.concatenate([hi, hi, lo], axis=1)


class Sizes:
    def __init__(self, n_gx, n_gy, n_gz, pair_dev):
        self.n_gx, self.n_gy, self.n_gz = n_gx, n_gy, n_gz
        self.nx, self.ny, self.nz = CX * n_gx, CY * n_gy, CZ * n_gz
        self.nky, self.nkz = self.ny // n_gx, self.nz // (n_gy * n_gz)
        self.pair_dev = pair_dev
        self.per = LANES // pair_dev
        self.groups = n_gx // self.per
        self.wide = max(self.nx, LANES)
        self.kys = self.wide // self.nx
        self.blocks = self.nky // self.kys
        self.cols = 2 * self.nkz * n_gy
        self.rows = self.nky * self.nx


def kz_start(z, gy, gz, dy):
    block = lax.rem(gy + dy, z.n_gy) * z.n_gz + gz
    return (block * z.nkz).astype(f32)


def put3(ref, rows, k, hi, lo, order):
    for n, which in enumerate(order):
        ref[rows, n * DEPTH + k * LANES : n * DEPTH + (k + 1) * LANES] = lo if which else hi


def chunk_work(z, place, prm, ytab, ztab, s):
    gx, gy, gz = place
    row = lambda a: prm[a : a + 1, :]
    cx, cy, cz, ox, oy, oz, rate, radius = [row(COEFS + n) for n in range(8)]
    nky, nkz, nx = z.nky, z.nkz, z.nx

    kyc = iota_f((nky, 1), 0) + (gx * nky).astype(f32)
    part = span_part(oy, rate, radius, ytab[...])
    pc, ps = cos_sin(kyc * cy * (1.0 / z.ny))
    fy = []
    for d in range(SIDE):
        a = part[:nky, d * LANES : (d + 1) * LANES]
        b = part[nky:, d * LANES : (d + 1) * LANES]
        fy.append((a * pc + b * ps, b * pc - a * ps))

    fx = factors(wrapped(iota_f((nx, LANES), 0), cx, float(z.nx)), ox, rate, radius)
    for k in range(SIDE):
        for i in range(SIDE):
            re = im = None
            for j in range(SIDE):
                c = row((i * SIDE + j) * SIDE + k)
                re = c * fy[j][0] if re is None else re + c * fy[j][0]
                im = c * fy[j][1] if im is None else im + c * fy[j][1]
            s.h[k * SIDE + i, :nky] = re
            s.h[k * SIDE + i, nky:] = im

    fxl = factors(
        wrapped(iota_f((CX, LANES), 0) + (gx * CX).astype(f32), cx, float(z.nx)), ox, rate, radius
    )
    fyl = factors(
        iota_f((CYW, LANES), 0) + ((gy * CY).astype(f32) - HALO) - cy, oy, rate, radius
    )
    fzl = factors(
        wrapped(iota_f((CZ, LANES), 0) + (gz * CZ).astype(f32), cz, float(z.nz)), oz, rate, radius
    )
    for k in range(SIDE):
        for j in range(SIDE):
            v = None
            for i in range(SIDE):
                w = row((i * SIDE + j) * SIDE + k) * fxl[i]
                v = w if v is None else v + w
            s.hd[k * SIDE + j] = v
        hi, lo = split(fzl[k])
        put3(s.zd, slice(0, CZ), k, hi, lo, (0, 0, 1))

    part = span_part(oz, rate, radius, ztab[...])
    n = z.n_gy * nkz
    low = iota_f((8, 1), 0)
    cb, sb = cos_sin(low * cz * (1.0 / z.nz))
    heads = jnp.concatenate(
        [iota_f((nkz // 8, 1), 0) * 8.0 + kz_start(z, gy, gz, dy) for dy in range(z.n_gy)], axis=0
    )
    s.ea[0], s.ea[1] = cos_sin(heads * cz * (1.0 / z.nz))
    pcs, pss = [], []
    for a in range(n // 8):
        ca, sa = s.ea[0, a : a + 1, :], s.ea[1, a : a + 1, :]
        pcs.append(ca * cb - sa * sb)
        pss.append(sa * cb + ca * sb)
    pc, ps = jnp.concatenate(pcs, axis=0), jnp.concatenate(pss, axis=0)
    for k in range(SIDE):
        a = part[:n, k * LANES : (k + 1) * LANES]
        b = part[n:, k * LANES : (k + 1) * LANES]
        for dy in range(z.n_gy):
            for m, v in enumerate((a * pc + b * ps, b * pc - a * ps)):
                hi, lo = split(v[dy * nkz : (dy + 1) * nkz])
                start = (2 * dy + m) * nkz
                put3(s.z, slice(start, start + nkz), k, hi, lo, (0, 0, 1))

    def build_cells():
        for x in range(CX):
            for k in range(SIDE):
                v = None
                for j in range(SIDE):
                    w = s.hd[k * SIDE + j, x : x + 1, :] * fyl[j]
                    v = w if v is None else v + w
                hi, lo = split(v)
                put3(s.d, slice(x * CYW, (x + 1) * CYW), k, hi, lo, (0, 1, 0))

    def build(g):
        t = s.t.at[g % 2]
        for m in range(2):
            for kk in range(z.kys):
                r = m * nky + g * z.kys + kk
                o = m * z.wide + kk * nx
                for k in range(SIDE):
                    v = None
                    for i in range(SIDE):
                        w = s.h[k * SIDE + i, r : r + 1, :] * fx[i]
                        v = w if v is None else v + w
                    hi, lo = split(v)
                    put3(t, slice(o, o + nx), k, hi, lo, (0, 1, 0))

    def add_cells():
        more = nt(s.d[...], s.zd[...])
        s.dacc[...] = s.dacc[...] + more.reshape(CX, CYW, CZ)

    def add(g):
        rows = slice(2 * z.wide * g, 2 * z.wide * (g + 1))
        s.acc[rows] = s.acc[rows] + nt(s.t[g % 2], s.z[...])

    build_cells()
    late = add_cells
    for g in range(z.blocks):
        build(g)
        late()
        late = functools.partial(add, g)
    late()


class Scratch:
    pass


def params_of(z, cells, offs, e_index, r_index, exponents, pm):
    n = z.pair_dev
    pm[...] = jnp.zeros_like(pm)
    radius = (HALO - r_index[...]).astype(f32)
    chosen = None
    for e in range(exponents.shape[0]):
        w = jnp.where(e_index[...] == e, exponents[e], 0.0)
        chosen = w if chosen is None else chosen + w
    pm[0:3, :n] = cells[...].astype(f32)
    pm[3:6, :n] = offs[...]
    pm[6:7, :n] = chosen / (radius * radius)
    pm[7:8, :n] = radius


def coefficients(z, basis, blocks):
    bh, bl = split(basis[...])
    ph, pb = split(blocks[...])
    ph = jnp.concatenate([ph] * FOLD, axis=0)
    pb = jnp.concatenate([pb] * FOLD, axis=0)
    both = nt(bh, ph) + (nt(bh, pb) + nt(bl, ph))
    lane = lax.broadcasted_iota(jnp.int32, (TOP, FOLD * z.pair_dev), 1) // z.pair_dev
    v = both[:TOP]
    for g in range(1, FOLD):
        v = jnp.where(lane == g, both[g * TOP : (g + 1) * TOP], v)
    return v


def unpack(z, blocks, prm):
    owner = lax.broadcasted_iota(jnp.int32, (TOP, LANES), 1) // z.pair_dev
    for g in range(FOLD):
        v = None
        for d, block in enumerate(blocks):
            shift = (d - g) % FOLD * z.pair_dev
            w = block[:TOP]
            w = pltpu.roll(w, shift, 1) if shift else w
            v = w if v is None else jnp.where(owner == d, w, v)
        prm[g * TOP : (g + 1) * TOP] = v
    v = None
    for d, block in enumerate(blocks):
        w = block[TOP:]
        w = pltpu.roll(w, d * z.pair_dev, 1) if d else w
        v = w if v is None else jnp.where(owner[:8] == d, w, v)
    prm[COEFS : COEFS + 8] = v


def swapped(z, b):
    lane = lax.broadcasted_iota(jnp.int32, (b.shape[0], LANES), 1)
    first = lane % (2 * z.nkz) < z.nkz
    out = []
    for c in range(z.cols // LANES):
        w = b[:, c * LANES : (c + 1) * LANES]
        down = pltpu.roll(w, LANES - z.nkz, 1)
        up = down if 2 * z.nkz == LANES else pltpu.roll(w, z.nkz, 1)
        out.append(jnp.where(first, down, -up))
    return jnp.concatenate(out, axis=1)


def kernel(
    z, basis_hbm, blocks_hbm, cells_hbm, offs_hbm, ei_hbm, ri_hbm, ex_hbm, xt_hbm,
    own, got, dacc, edges,
    basis, blocks, cells, offs, e_index, r_index, exponents, xt, pm, prm, cols, give,
    h, hd, ea, acc,
    in_sem, send_z, recv_z, send_c, recv_c, send_e, recv_e, send_d, recv_d,
):
    n_gx, n_gy, n_gz = z.n_gx, z.n_gy, z.n_gz
    gx, gy, gz = (lax.axis_index(a) for a in ("gx", "gy", "gz"))
    place = gx, gy, gz
    mesh_type = pl.DeviceIdType.MESH

    def along_z(r):
        return gx, gy, lax.rem(gz + n_gz - r, n_gz)

    def along_x(dx):
        return lax.rem(gx + n_gx - dx, n_gx), gy, gz

    def along_y(dy):
        return gx, lax.rem(gy + n_gy + dy, n_gy), gz

    barrier = pltpu.get_barrier_semaphore()
    for r in range(1, n_gz):
        pl.semaphore_signal(barrier, inc=1, device_id=along_z(r), device_id_type=mesh_type)

    def greet(dx, carry):
        pl.semaphore_signal(barrier, inc=1, device_id=along_x(dx), device_id_type=mesh_type)
        return carry

    lax.fori_loop(1, n_gx, greet, 0)
    for dy in range(1, n_gy):
        pl.semaphore_signal(barrier, inc=1, device_id=along_y(dy), device_id_type=mesh_type)

    pairs = [
        (blocks_hbm, blocks), (basis_hbm, basis), (cells_hbm, cells), (offs_hbm, offs),
        (ei_hbm, e_index), (ri_hbm, r_index), (ex_hbm, exponents), (xt_hbm, xt),
    ]
    loads = [
        pltpu.make_async_copy(a, b, in_sem.at[n]) for n, (a, b) in enumerate(pairs)
    ]
    for c in loads:
        c.start()
    for c in loads[:-1]:
        c.wait()
    params_of(z, cells, offs, e_index, r_index, exponents, pm)
    cols[0, 0, :TOP] = coefficients(z, basis, blocks)
    cols[0, 0, TOP:] = pm[...]

    def body(ytab, ztab, t, zs, d, zd):
        s = Scratch()
        s.t, s.z, s.d, s.zd, s.h, s.hd, s.ea, s.acc, s.dacc = t, zs, d, zd, h, hd, ea, acc, dacc
        kyc = iota_f((z.nky, 1), 0) + (gx * z.nky).astype(f32)
        kzc = jnp.concatenate(
            [iota_f((z.nkz, 1), 0) + kz_start(z, gy, gz, dy) for dy in range(n_gy)], axis=0
        )
        ytab[...] = span_table(kyc, z.ny)
        ztab[...] = span_table(kzc, z.nz)
        for ref in (acc, dacc):
            ref[...] = jnp.zeros_like(ref)
        pl.semaphore_wait(barrier, n_gz + n_gx + n_gy - 3)

        def copy_z(r):
            return pltpu.make_async_remote_copy(
                src_ref=cols.at[0, 0],
                dst_ref=cols.at[r, 0],
                send_sem=send_z.at[r],
                recv_sem=recv_z.at[r],
                device_id=along_z(r),
                device_id_type=mesh_type,
            )

        def copy_c(r, dx):
            return pltpu.make_async_remote_copy(
                src_ref=cols.at[r, 0],
                dst_ref=cols.at[r, dx],
                send_sem=send_c.at[r * n_gx + dx],
                recv_sem=recv_c.at[r * n_gx + dx],
                device_id=along_x(dx),
                device_id_type=mesh_type,
            )

        def forward(r):
            def one(dx, carry):
                copy_c(r, dx).start()
                return carry

            lax.fori_loop(1, n_gx, one, 0)

        for r in range(1, n_gz):
            copy_z(r).start()
        forward(0)
        for r in range(1, n_gz - 1):
            copy_z(r).wait_recv()
            forward(r)

        def step(c, carry):
            r, g = c // z.groups, c % z.groups

            @pl.when(c == z.groups)
            def _():
                copy_z(n_gz - 1).wait_recv()
                forward(n_gz - 1)

            for d in range(z.per):
                dx = g * z.per + d

                @pl.when(dx > 0)
                def _(dx=dx):
                    copy_c(r, dx).wait_recv()

            unpack(z, [cols[r, g * z.per + d] for d in range(z.per)], prm)
            chunk_work(z, place, prm, ytab, ztab, s)
            return carry

        lax.fori_loop(0, n_gz * z.groups, step, 0)

        def copy_d(which):
            return pltpu.make_async_remote_copy(
                src_ref=dacc.at[:, pl.ds(which * (CY + HALO), HALO), :],
                dst_ref=edges.at[which],
                send_sem=send_d.at[which],
                recv_sem=recv_d.at[which],
                device_id=along_y(2 * which - 1),
                device_id_type=mesh_type,
            )

        def copy_e(dy, g):
            rows = pl.ds(g * z.wide, z.wide)
            return pltpu.make_async_remote_copy(
                src_ref=give.at[dy - 1, rows],
                dst_ref=got.at[dy - 1, rows],
                send_sem=send_e.at[dy * z.blocks + g],
                recv_sem=recv_e.at[dy * z.blocks + g],
                device_id=along_y(dy),
                device_id_type=mesh_type,
            )

        loads[-1].wait()
        for g in range(z.blocks):
            hi, lo = split(acc[2 * z.wide * g : 2 * z.wide * (g + 1)])
            q = jnp.dot(
                xt[...], jnp.concatenate([hi, lo, hi], axis=0), preferred_element_type=f32
            )
            out = q[: z.wide] + swapped(z, q[z.wide :])
            rows = slice(g * z.wide, (g + 1) * z.wide)
            own[rows] = out[:, : 2 * z.nkz]
            for dy in range(1, n_gy):
                give[dy - 1, rows] = out[:, 2 * z.nkz * dy : 2 * z.nkz * (dy + 1)]
            if g == 0:
                for which in range(2):
                    copy_d(which).start()
            else:
                for dy in range(1, n_gy):
                    copy_e(dy, g - 1).start()
        for dy in range(1, n_gy):
            copy_e(dy, z.blocks - 1).start()
        for r in range(1, n_gz):
            copy_z(r).wait_send()

        def drain(c, carry):
            @pl.when(c % n_gx > 0)
            def _():
                copy_c(c // n_gx, c % n_gx).wait_send()

            return carry

        lax.fori_loop(0, n_gz * n_gx, drain, 0)
        for which in range(2):
            copy_d(which).wait()
        for g in range(z.blocks):
            for dy in range(1, n_gy):
                copy_e(dy, g).wait()

    pl.run_scoped(
        body,
        pltpu.VMEM((2 * z.nky, 3 * SPAN), bf16),
        pltpu.VMEM((z.cols, 3 * SPAN), bf16),
        pltpu.VMEM((2, 2 * z.wide, 3 * DEPTH), bf16),
        pltpu.VMEM((z.cols, 3 * DEPTH), bf16),
        pltpu.VMEM((CX * CYW, 3 * DEPTH), bf16),
        pltpu.VMEM((CZ, 3 * DEPTH), bf16),
    )


def finish(z, own, got, dacc, edges, dens_ref, spec_ref):
    total = own[...]
    for dy in range(1, z.n_gy):
        total = total + got[dy - 1]
    spec_ref[0] = total[:, : z.nkz]
    spec_ref[1] = total[:, z.nkz :]
    dens_ref[...] = dacc[:, HALO : HALO + CY]
    dens_ref[:, CY - HALO :] = dens_ref[:, CY - HALO :] + edges[0]
    dens_ref[:, :HALO] = dens_ref[:, :HALO] + edges[1]


def x_table(z):
    idx = np.arange(z.nx)
    angle = (idx[:, None] * idx[None, :] % z.nx) * (2.0 * math.pi / z.nx)
    eye = np.eye(z.kys)
    c, s = np.kron(eye, np.cos(angle)), np.kron(eye, np.sin(angle))
    full = np.block([[c, s], [s, -c]]) / math.sqrt(z.nx * z.ny * z.nz)
    full = full.astype(np.float32)
    hi = full.astype(ml_dtypes.bfloat16)
    lo = (full - hi.astype(np.float32)).astype(ml_dtypes.bfloat16)
    return np.concatenate([hi, hi, lo], axis=1)


def shards(
    pair_blocks, basis_map, pair_cells, pair_offsets, exponent_index, radius_index, exponents
):
    n_gx, n_gy, n_gz = (lax.axis_size(a) for a in ("gx", "gy", "gz"))
    pair_dev = pair_blocks.shape[1]
    z = Sizes(n_gx, n_gy, n_gz, pair_dev)
    assert FOLD * pair_dev == LANES and n_gx % z.per == 0 and n_gz >= 3 and n_gy >= 2
    in_vmem = pl.BlockSpec(memory_space=pltpu.VMEM)
    in_hbm = pl.BlockSpec(memory_space=pl.ANY)
    basis = basis_map.T
    blocks = pair_blocks.T
    xt = jnp.asarray(x_table(z))
    ei, ri = exponent_index.reshape(1, -1), radius_index.reshape(1, -1)
    dma = pltpu.SemaphoreType.DMA
    own, got, dacc, edges = pl.pallas_call(
        functools.partial(kernel, z),
        out_shape=[
            jax.ShapeDtypeStruct((z.rows, 2 * z.nkz), f32),
            jax.ShapeDtypeStruct((n_gy - 1, z.rows, 2 * z.nkz), f32),
            jax.ShapeDtypeStruct((CX, CYW, CZ), f32),
            jax.ShapeDtypeStruct((2, CX, HALO, CZ), f32),
        ],
        in_specs=[in_hbm] * 8,
        out_specs=[in_vmem] * 4,
        scratch_shapes=[
            pltpu.VMEM(basis.shape, f32),
            pltpu.VMEM(blocks.shape, f32),
            pltpu.VMEM(pair_cells.shape, jnp.int32),
            pltpu.VMEM(pair_offsets.shape, f32),
            pltpu.VMEM(ei.shape, jnp.int32),
            pltpu.VMEM(ri.shape, jnp.int32),
            pltpu.SMEM(exponents.shape, f32),
            pltpu.VMEM(xt.shape, bf16),
            pltpu.VMEM((8, LANES), f32),
            pltpu.VMEM((COEFS + 8, LANES), f32),
            pltpu.VMEM((n_gz, n_gx, BLOCK_ROWS, LANES), f32),
            pltpu.VMEM((n_gy - 1, z.rows, 2 * z.nkz), f32),
            pltpu.VMEM((SIDE * SIDE, 2 * z.nky, LANES), f32),
            pltpu.VMEM((SIDE * SIDE, CX, LANES), f32),
            pltpu.VMEM((2, n_gy * z.nkz // 8, LANES), f32),
            pltpu.VMEM((2 * z.rows, z.cols), f32),
            dma((8,)),
            dma((n_gz,)),
            dma((n_gz,)),
            dma((n_gz * n_gx,)),
            dma((n_gz * n_gx,)),
            dma((n_gy * z.blocks,)),
            dma((n_gy * z.blocks,)),
            dma((2,)),
            dma((2,)),
        ],
        compiler_params=pltpu.CompilerParams(
            collective_id=0, has_side_effects=True, vmem_limit_bytes=VMEM_LIMIT
        ),
    )(basis, blocks, pair_cells, pair_offsets, ei, ri, exponents, xt)
    dens, spec = pl.pallas_call(
        functools.partial(finish, z),
        out_shape=[
            jax.ShapeDtypeStruct((CX, CY, CZ), f32),
            jax.ShapeDtypeStruct((2, z.rows, z.nkz), f32),
        ],
        in_specs=[in_vmem] * 4,
        out_specs=[in_vmem] * 2,
        compiler_params=pltpu.CompilerParams(vmem_limit_bytes=VMEM_LIMIT),
    )(own, got, dacc, edges)
    return dens, spec.reshape(2, z.nky, z.nx, z.nkz).transpose(0, 3, 1, 2)


def solution(mesh):
    placed = (
        P(None, ("gx", "gy", "gz")),
        P(),
        P(None, ("gx", "gy", "gz")),
        P(None, ("gx", "gy", "gz")),
        P(("gx", "gy", "gz")),
        P(("gx", "gy", "gz")),
        P(),
    )
    return jax.shard_map(
        shards,
        mesh=mesh,
        in_specs=placed,
        out_specs=(P("gx", "gy", "gz"), P(None, ("gy", "gz"), "gx", None)),
        check_vma=False,
    )
```

```python
import functools
import math

import jax
import jax.numpy as jnp
import ml_dtypes
import numpy as np
from jax import lax
from jax.experimental import pallas as pl
from jax.experimental.pallas import tpu as pltpu
from jax.sharding import PartitionSpec as P

DEG = 3
HALO = 8
CX = 8
CY = 32
CZ = 128
SIDE = DEG + 1
LANES = 128
SPAN = 32
VMEM_LIMIT = 40 << 20
COEFS = SIDE**3
FOLD = 4
TOP = COEFS // FOLD
BLOCK_ROWS = TOP + 8
CYW = CY + 2 * HALO
DEPTH = SIDE * LANES

f32 = jnp.float32
bf16 = jnp.bfloat16


def iota_f(shape, dim):
    return lax.broadcasted_iota(jnp.int32, shape, dim).astype(f32)


def cos_sin(turns):
    r = turns - jnp.floor(turns + 0.5)
    t = r * math.pi
    t2 = t * t
    s = t * _poly(t2, [(-1) ** n / math.factorial(2 * n + 1) for n in range(7)])
    c = _poly(t2, [(-1) ** n / math.factorial(2 * n) for n in range(8)])
    return 1.0 - 2.0 * s * s, 2.0 * s * c


def _poly(x, coefs):
    out = jnp.full_like(x, coefs[-1])
    for a in reversed(coefs[:-1]):
        out = out * x + a
    return out


def wrapped(cells, centre, total):
    d = cells - centre
    d = jnp.where(d < -HALO, d + total, d)
    return jnp.where(d > total - 1 - HALO, d - total, d)


def factors(offset, within, rate, radius):
    u = offset - within
    env = jnp.where(jnp.abs(offset) <= radius, jnp.exp(-rate * u * u), 0.0)
    s = u * (1.0 / HALO)
    out = [env]
    for _ in range(DEG):
        out.append(out[-1] * s)
    return out


def split(v):
    hi = v.astype(bf16)
    return hi, (v - hi.astype(f32)).astype(bf16)


def nt(a, b):
    return lax.dot_general(a, b, (((1,), (1,)), ((), ())), preferred_element_type=f32)


def span_part(within, rate, radius, table):
    offs = iota_f((SPAN, LANES), 0) - HALO
    four = jnp.concatenate(factors(offs, within, rate, radius), axis=1)
    hi, lo = split(four)
    return jnp.dot(table, jnp.concatenate([hi, lo, hi], axis=0), preferred_element_type=f32)


def span_table(frequency, length):
    offs = iota_f((1, SPAN), 1) - HALO
    c, s = cos_sin(frequency * offs * (1.0 / length))
    hi, lo = split(jnp.concatenate([c, -s], axis=0))
    return jnp.concatenate([hi, hi, lo], axis=1)


class Sizes:
    def __init__(self, n_gx, n_gy, n_gz, pair_dev):
        self.n_gx, self.n_gy, self.n_gz = n_gx, n_gy, n_gz
        self.nx, self.ny, self.nz = CX * n_gx, CY * n_gy, CZ * n_gz
        self.nky, self.nkz = self.ny // n_gx, self.nz // (n_gy * n_gz)
        self.pair_dev = pair_dev
        self.per = LANES // pair_dev
        self.groups = n_gx // self.per
        self.wide = max(self.nx, LANES)
        self.kys = self.wide // self.nx
        self.blocks = self.nky // self.kys
        self.cols = 2 * self.nkz * n_gy
        self.rows = self.nky * self.nx


def kz_start(z, gy, gz, dy):
    block = lax.rem(gy + dy, z.n_gy) * z.n_gz + gz
    return (block * z.nkz).astype(f32)


def put3(ref, rows, k, hi, lo, order):
    for n, which in enumerate(order):
        ref[rows, n * DEPTH + k * LANES : n * DEPTH + (k + 1) * LANES] = lo if which else hi


def chunk_work(z, place, prm, ytab, ztab, s):
    gx, gy, gz = place
    row = lambda a: prm[a : a + 1, :]
    cx, cy, cz, ox, oy, oz, rate, radius = [row(COEFS + n) for n in range(8)]
    nky, nkz, nx = z.nky, z.nkz, z.nx

    kyc = iota_f((nky, 1), 0) + (gx * nky).astype(f32)
    part = span_part(oy, rate, radius, ytab[...])
    pc, ps = cos_sin(kyc * cy * (1.0 / z.ny))
    fy = []
    for d in range(SIDE):
        a = part[:nky, d * LANES : (d + 1) * LANES]
        b = part[nky:, d * LANES : (d + 1) * LANES]
        fy.append((a * pc + b * ps, b * pc - a * ps))

    fx = factors(wrapped(iota_f((nx, LANES), 0), cx, float(z.nx)), ox, rate, radius)
    for k in range(SIDE):
        for i in range(SIDE):
            re = im = None
            for j in range(SIDE):
                c = row((i * SIDE + j) * SIDE + k)
                re = c * fy[j][0] if re is None else re + c * fy[j][0]
                im = c * fy[j][1] if im is None else im + c * fy[j][1]
            s.h[k * SIDE + i, :nky] = re
            s.h[k * SIDE + i, nky:] = im

    fxl = factors(
        wrapped(iota_f((CX, LANES), 0) + (gx * CX).astype(f32), cx, float(z.nx)), ox, rate, radius
    )
    fyl = factors(
        iota_f((CYW, LANES), 0) + ((gy * CY).astype(f32) - HALO) - cy, oy, rate, radius
    )
    fzl = factors(
        wrapped(iota_f((CZ, LANES), 0) + (gz * CZ).astype(f32), cz, float(z.nz)), oz, rate, radius
    )
    for k in range(SIDE):
        for j in range(SIDE):
            v = None
            for i in range(SIDE):
                w = row((i * SIDE + j) * SIDE + k) * fxl[i]
                v = w if v is None else v + w
            s.hd[k * SIDE + j] = v
        hi, lo = split(fzl[k])
        put3(s.zd, slice(0, CZ), k, hi, lo, (0, 0, 1))

    part = span_part(oz, rate, radius, ztab[...])
    n = z.n_gy * nkz
    low = iota_f((8, 1), 0)
    cb, sb = cos_sin(low * cz * (1.0 / z.nz))
    heads = jnp.concatenate(
        [iota_f((nkz // 8, 1), 0) * 8.0 + kz_start(z, gy, gz, dy) for dy in range(z.n_gy)], axis=0
    )
    s.ea[0], s.ea[1] = cos_sin(heads * cz * (1.0 / z.nz))
    pcs, pss = [], []
    for a in range(n // 8):
        ca, sa = s.ea[0, a : a + 1, :], s.ea[1, a : a + 1, :]
        pcs.append(ca * cb - sa * sb)
        pss.append(sa * cb + ca * sb)
    pc, ps = jnp.concatenate(pcs, axis=0), jnp.concatenate(pss, axis=0)
    for k in range(SIDE):
        a = part[:n, k * LANES : (k + 1) * LANES]
        b = part[n:, k * LANES : (k + 1) * LANES]
        for dy in range(z.n_gy):
            for m, v in enumerate((a * pc + b * ps, b * pc - a * ps)):
                hi, lo = split(v[dy * nkz : (dy + 1) * nkz])
                start = (2 * dy + m) * nkz
                put3(s.z, slice(start, start + nkz), k, hi, lo, (0, 0, 1))

    def build_cells():
        for x in range(CX):
            for k in range(SIDE):
                v = None
                for j in range(SIDE):
                    w = s.hd[k * SIDE + j, x : x + 1, :] * fyl[j]
                    v = w if v is None else v + w
                hi, lo = split(v)
                put3(s.d, slice(x * CYW, (x + 1) * CYW), k, hi, lo, (0, 1, 0))

    def build(g):
        t = s.t.at[g % 2]
        for m in range(2):
            for kk in range(z.kys):
                r = m * nky + g * z.kys + kk
                o = m * z.wide + kk * nx
                for k in range(SIDE):
                    v = None
                    for i in range(SIDE):
                        w = s.h[k * SIDE + i, r : r + 1, :] * fx[i]
                        v = w if v is None else v + w
                    hi, lo = split(v)
                    put3(t, slice(o, o + nx), k, hi, lo, (0, 1, 0))

    def add_cells():
        more = nt(s.d[...], s.zd[...])
        s.dacc[...] = s.dacc[...] + more.reshape(CX, CYW, CZ)

    def add(g):
        rows = slice(2 * z.wide * g, 2 * z.wide * (g + 1))
        s.acc[rows] = s.acc[rows] + nt(s.t[g % 2], s.z[...])

    build_cells()
    late = add_cells
    for g in range(z.blocks):
        build(g)
        late()
        late = functools.partial(add, g)
    late()


class Scratch:
    pass


def params_of(z, cells, offs, e_index, r_index, exponents, pm):
    n = z.pair_dev
    pm[...] = jnp.zeros_like(pm)
    radius = (HALO - r_index[...]).astype(f32)
    chosen = None
    for e in range(exponents.shape[0]):
        w = jnp.where(e_index[...] == e, exponents[e], 0.0)
        chosen = w if chosen is None else chosen + w
    pm[0:3, :n] = cells[...].astype(f32)
    pm[3:6, :n] = offs[...]
    pm[6:7, :n] = chosen / (radius * radius)
    pm[7:8, :n] = radius


def coefficients(z, basis, blocks):
    bh, bl = split(basis[...])
    ph, pb = split(blocks[...])
    ph = jnp.concatenate([ph] * FOLD, axis=0)
    pb = jnp.concatenate([pb] * FOLD, axis=0)
    both = nt(bh, ph) + (nt(bh, pb) + nt(bl, ph))
    lane = lax.broadcasted_iota(jnp.int32, (TOP, FOLD * z.pair_dev), 1) // z.pair_dev
    v = both[:TOP]
    for g in range(1, FOLD):
        v = jnp.where(lane == g, both[g * TOP : (g + 1) * TOP], v)
    return v


def unpack(z, blocks, prm):
    owner = lax.broadcasted_iota(jnp.int32, (TOP, LANES), 1) // z.pair_dev
    for g in range(FOLD):
        v = None
        for d, block in enumerate(blocks):
            shift = (d - g) % FOLD * z.pair_dev
            w = block[:TOP]
            w = pltpu.roll(w, shift, 1) if shift else w
            v = w if v is None else jnp.where(owner == d, w, v)
        prm[g * TOP : (g + 1) * TOP] = v
    v = None
    for d, block in enumerate(blocks):
        w = block[TOP:]
        w = pltpu.roll(w, d * z.pair_dev, 1) if d else w
        v = w if v is None else jnp.where(owner[:8] == d, w, v)
    prm[COEFS : COEFS + 8] = v


def swapped(z, b):
    lane = lax.broadcasted_iota(jnp.int32, (b.shape[0], LANES), 1)
    first = lane % (2 * z.nkz) < z.nkz
    out = []
    for c in range(z.cols // LANES):
        w = b[:, c * LANES : (c + 1) * LANES]
        down = pltpu.roll(w, LANES - z.nkz, 1)
        up = down if 2 * z.nkz == LANES else pltpu.roll(w, z.nkz, 1)
        out.append(jnp.where(first, down, -up))
    return jnp.concatenate(out, axis=1)


def kernel(
    z, basis_hbm, blocks_hbm, cells_hbm, offs_hbm, ei_hbm, ri_hbm, ex_hbm, xt_hbm,
    own, got, dacc, edges,
    basis, blocks, cells, offs, e_index, r_index, exponents, xt, pm, prm, cols, give,
    h, hd, ea, acc,
    in_sem, send_z, recv_z, send_c, recv_c, send_e, recv_e, send_d, recv_d,
):
    n_gx, n_gy, n_gz = z.n_gx, z.n_gy, z.n_gz
    gx, gy, gz = (lax.axis_index(a) for a in ("gx", "gy", "gz"))
    place = gx, gy, gz
    mesh_type = pl.DeviceIdType.MESH

    def along_z(r):
        return gx, gy, lax.rem(gz + n_gz - r, n_gz)

    def along_x(dx):
        return lax.rem(gx + n_gx - dx, n_gx), gy, gz

    def along_y(dy):
        return gx, lax.rem(gy + n_gy + dy, n_gy), gz

    barrier = pltpu.get_barrier_semaphore()
    for r in range(1, n_gz):
        pl.semaphore_signal(barrier, inc=1, device_id=along_z(r), device_id_type=mesh_type)

    def greet(dx, carry):
        pl.semaphore_signal(barrier, inc=1, device_id=along_x(dx), device_id_type=mesh_type)
        return carry

    lax.fori_loop(1, n_gx, greet, 0)
    for dy in range(1, n_gy):
        pl.semaphore_signal(barrier, inc=1, device_id=along_y(dy), device_id_type=mesh_type)

    pairs = [
        (blocks_hbm, blocks), (basis_hbm, basis), (cells_hbm, cells), (offs_hbm, offs),
        (ei_hbm, e_index), (ri_hbm, r_index), (ex_hbm, exponents), (xt_hbm, xt),
    ]
    loads = [
        pltpu.make_async_copy(a, b, in_sem.at[n]) for n, (a, b) in enumerate(pairs)
    ]
    for c in loads:
        c.start()
    for c in loads[:-1]:
        c.wait()
    params_of(z, cells, offs, e_index, r_index, exponents, pm)
    cols[0, 0, :TOP] = coefficients(z, basis, blocks)
    cols[0, 0, TOP:] = pm[...]

    def body(ytab, ztab, t, zs, d, zd):
        s = Scratch()
        s.t, s.z, s.d, s.zd, s.h, s.hd, s.ea, s.acc, s.dacc = t, zs, d, zd, h, hd, ea, acc, dacc
        kyc = iota_f((z.nky, 1), 0) + (gx * z.nky).astype(f32)
        kzc = jnp.concatenate(
            [iota_f((z.nkz, 1), 0) + kz_start(z, gy, gz, dy) for dy in range(n_gy)], axis=0
        )
        ytab[...] = span_table(kyc, z.ny)
        ztab[...] = span_table(kzc, z.nz)
        for ref in (acc, dacc):
            ref[...] = jnp.zeros_like(ref)
        pl.semaphore_wait(barrier, n_gz + n_gx + n_gy - 3)

        def copy_z(r):
            return pltpu.make_async_remote_copy(
                src_ref=cols.at[0, 0],
                dst_ref=cols.at[r, 0],
                send_sem=send_z.at[r],
                recv_sem=recv_z.at[r],
                device_id=along_z(r),
                device_id_type=mesh_type,
            )

        def copy_c(r, dx):
            return pltpu.make_async_remote_copy(
                src_ref=cols.at[r, 0],
                dst_ref=cols.at[r, dx],
                send_sem=send_c.at[r * n_gx + dx],
                recv_sem=recv_c.at[r * n_gx + dx],
                device_id=along_x(dx),
                device_id_type=mesh_type,
            )

        def forward(r):
            def one(dx, carry):
                copy_c(r, dx).start()
                return carry

            lax.fori_loop(1, n_gx, one, 0)

        for r in range(1, n_gz):
            copy_z(r).start()
        forward(0)
        for r in range(1, n_gz - 1):
            copy_z(r).wait_recv()
            forward(r)

        def step(c, carry):
            r, g = c // z.groups, c % z.groups

            @pl.when(c == z.groups)
            def _():
                copy_z(n_gz - 1).wait_recv()
                forward(n_gz - 1)

            for d in range(z.per):
                dx = g * z.per + d

                @pl.when(dx > 0)
                def _(dx=dx):
                    copy_c(r, dx).wait_recv()

            unpack(z, [cols[r, g * z.per + d] for d in range(z.per)], prm)
            chunk_work(z, place, prm, ytab, ztab, s)
            return carry

        lax.fori_loop(0, n_gz * z.groups, step, 0)

        def copy_d(which):
            return pltpu.make_async_remote_copy(
                src_ref=dacc.at[:, pl.ds(which * (CY + HALO), HALO), :],
                dst_ref=edges.at[which],
                send_sem=send_d.at[which],
                recv_sem=recv_d.at[which],
                device_id=along_y(2 * which - 1),
                device_id_type=mesh_type,
            )

        def copy_e(dy, g):
            rows = pl.ds(g * z.wide, z.wide)
            return pltpu.make_async_remote_copy(
                src_ref=give.at[dy - 1, rows],
                dst_ref=got.at[dy - 1, rows],
                send_sem=send_e.at[dy * z.blocks + g],
                recv_sem=recv_e.at[dy * z.blocks + g],
                device_id=along_y(dy),
                device_id_type=mesh_type,
            )

        loads[-1].wait()
        for g in range(z.blocks):
            hi, lo = split(acc[2 * z.wide * g : 2 * z.wide * (g + 1)])
            q = jnp.dot(
                xt[...], jnp.concatenate([hi, lo, hi], axis=0), preferred_element_type=f32
            )
            out = q[: z.wide] + swapped(z, q[z.wide :])
            rows = slice(g * z.wide, (g + 1) * z.wide)
            own[rows] = out[:, : 2 * z.nkz]
            for dy in range(1, n_gy):
                give[dy - 1, rows] = out[:, 2 * z.nkz * dy : 2 * z.nkz * (dy + 1)]
            if g == 0:
                for which in range(2):
                    copy_d(which).start()
            else:
                for dy in range(1, n_gy):
                    copy_e(dy, g - 1).start()
        for dy in range(1, n_gy):
            copy_e(dy, z.blocks - 1).start()
        for r in range(1, n_gz):
            copy_z(r).wait_send()

        def drain(c, carry):
            @pl.when(c % n_gx > 0)
            def _():
                copy_c(c // n_gx, c % n_gx).wait_send()

            return carry

        lax.fori_loop(0, n_gz * n_gx, drain, 0)
        for which in range(2):
            copy_d(which).wait()
        for g in range(z.blocks):
            for dy in range(1, n_gy):
                copy_e(dy, g).wait()

    pl.run_scoped(
        body,
        pltpu.VMEM((2 * z.nky, 3 * SPAN), bf16),
        pltpu.VMEM((z.cols, 3 * SPAN), bf16),
        pltpu.VMEM((2, 2 * z.wide, 3 * DEPTH), bf16),
        pltpu.VMEM((z.cols, 3 * DEPTH), bf16),
        pltpu.VMEM((CX * CYW, 3 * DEPTH), bf16),
        pltpu.VMEM((CZ, 3 * DEPTH), bf16),
    )


def finish(z, own, got, dacc, edges, dens_ref, spec_ref):
    total = own[...]
    for dy in range(1, z.n_gy):
        total = total + got[dy - 1]
    spec_ref[0] = total[:, : z.nkz]
    spec_ref[1] = total[:, z.nkz :]
    dens_ref[...] = dacc[:, HALO : HALO + CY]
    dens_ref[:, CY - HALO :] = dens_ref[:, CY - HALO :] + edges[0]
    dens_ref[:, :HALO] = dens_ref[:, :HALO] + edges[1]


def x_table(z):
    idx = np.arange(z.nx)
    angle = (idx[:, None] * idx[None, :] % z.nx) * (2.0 * math.pi / z.nx)
    eye = np.eye(z.kys)
    c, s = np.kron(eye, np.cos(angle)), np.kron(eye, np.sin(angle))
    full = np.block([[c, s], [s, -c]]) / math.sqrt(z.nx * z.ny * z.nz)
    full = full.astype(np.float32)
    hi = full.astype(ml_dtypes.bfloat16)
    lo = (full - hi.astype(np.float32)).astype(ml_dtypes.bfloat16)
    return np.concatenate([hi, hi, lo], axis=1)


def shards(
    pair_blocks, basis_map, pair_cells, pair_offsets, exponent_index, radius_index, exponents
):
    n_gx, n_gy, n_gz = (lax.axis_size(a) for a in ("gx", "gy", "gz"))
    pair_dev = pair_blocks.shape[1]
    z = Sizes(n_gx, n_gy, n_gz, pair_dev)
    assert FOLD * pair_dev == LANES and n_gx % z.per == 0 and n_gz >= 3 and n_gy >= 2
    in_vmem = pl.BlockSpec(memory_space=pltpu.VMEM)
    in_hbm = pl.BlockSpec(memory_space=pltpu.HBM)
    basis = basis_map.T
    blocks = pair_blocks.T
    xt = jnp.asarray(x_table(z))
    ei, ri = exponent_index.reshape(1, -1), radius_index.reshape(1, -1)
    dma = pltpu.SemaphoreType.DMA
    own, got, dacc, edges = pl.pallas_call(
        functools.partial(kernel, z),
        out_shape=[
            jax.ShapeDtypeStruct((z.rows, 2 * z.nkz), f32),
            jax.ShapeDtypeStruct((n_gy - 1, z.rows, 2 * z.nkz), f32),
            jax.ShapeDtypeStruct((CX, CYW, CZ), f32),
            jax.ShapeDtypeStruct((2, CX, HALO, CZ), f32),
        ],
        in_specs=[in_hbm] * 8,
        out_specs=[in_vmem] * 4,
        scratch_shapes=[
            pltpu.VMEM(basis.shape, f32),
            pltpu.VMEM(blocks.shape, f32),
            pltpu.VMEM(pair_cells.shape, jnp.int32),
            pltpu.VMEM(pair_offsets.shape, f32),
            pltpu.VMEM(ei.shape, jnp.int32),
            pltpu.VMEM(ri.shape, jnp.int32),
            pltpu.SMEM(exponents.shape, f32),
            pltpu.VMEM(xt.shape, bf16),
            pltpu.VMEM((8, LANES), f32),
            pltpu.VMEM((COEFS + 8, LANES), f32),
            pltpu.VMEM((n_gz, n_gx, BLOCK_ROWS, LANES), f32),
            pltpu.VMEM((n_gy - 1, z.rows, 2 * z.nkz), f32),
            pltpu.VMEM((SIDE * SIDE, 2 * z.nky, LANES), f32),
            pltpu.VMEM((SIDE * SIDE, CX, LANES), f32),
            pltpu.VMEM((2, n_gy * z.nkz // 8, LANES), f32),
            pltpu.VMEM((2 * z.rows, z.cols), f32),
            dma((8,)),
            dma((n_gz,)),
            dma((n_gz,)),
            dma((n_gz * n_gx,)),
            dma((n_gz * n_gx,)),
            dma((n_gy * z.blocks,)),
            dma((n_gy * z.blocks,)),
            dma((2,)),
            dma((2,)),
        ],
        compiler_params=pltpu.CompilerParams(
            collective_id=0, has_side_effects=True, vmem_limit_bytes=VMEM_LIMIT
        ),
    )(
        *(
            pltpu.with_memory_space_constraint(a, pltpu.HBM)
            for a in (basis, blocks, pair_cells, pair_offsets, ei, ri, exponents, xt)
        )
    )
    dens, spec = pl.pallas_call(
        functools.partial(finish, z),
        out_shape=[
            jax.ShapeDtypeStruct((CX, CY, CZ), f32),
            jax.ShapeDtypeStruct((2, z.rows, z.nkz), f32),
        ],
        in_specs=[in_vmem] * 4,
        out_specs=[in_vmem] * 2,
        compiler_params=pltpu.CompilerParams(vmem_limit_bytes=VMEM_LIMIT),
    )(own, got, dacc, edges)
    return dens, spec.reshape(2, z.nky, z.nx, z.nkz).transpose(0, 3, 1, 2)


def solution(mesh):
    placed = (
        P(None, ("gx", "gy", "gz")),
        P(),
        P(None, ("gx", "gy", "gz")),
        P(None, ("gx", "gy", "gz")),
        P(("gx", "gy", "gz")),
        P(("gx", "gy", "gz")),
        P(),
    )
    return jax.shard_map(
        shards,
        mesh=mesh,
        in_specs=placed,
        out_specs=(P("gx", "gy", "gz"), P(None, ("gy", "gz"), "gx", None)),
        check_vma=False,
    )
```

```python
import functools
import math

import jax
import jax.numpy as jnp
import ml_dtypes
import numpy as np
from jax import lax
from jax.experimental import pallas as pl
from jax.experimental.pallas import tpu as pltpu
from jax.sharding import PartitionSpec as P

DEG = 3
HALO = 8
CX = 8
CY = 32
CZ = 128
SIDE = DEG + 1
LANES = 128
VMEM_LIMIT = 40 << 20
COEFS = SIDE**3
FOLD = 4
TOP = COEFS // FOLD
BLOCK_ROWS = TOP + 8
CYW = CY + 2 * HALO
CZW = CZ + 2 * HALO
TS = 4
DEPTH = SIDE * LANES

f32 = jnp.float32
bf16 = jnp.bfloat16


def iota_f(shape, dim):
    return lax.broadcasted_iota(jnp.int32, shape, dim).astype(f32)


def cos_sin(turns):
    r = turns - jnp.floor(turns + 0.5)
    t = r * math.pi
    t2 = t * t
    s = t * _poly(t2, [(-1) ** n / math.factorial(2 * n + 1) for n in range(7)])
    c = _poly(t2, [(-1) ** n / math.factorial(2 * n) for n in range(8)])
    return 1.0 - 2.0 * s * s, 2.0 * s * c


def _poly(x, coefs):
    out = jnp.full_like(x, coefs[-1])
    for a in reversed(coefs[:-1]):
        out = out * x + a
    return out


def wrapped(cells, centre, total):
    d = cells - centre
    d = jnp.where(d < -HALO, d + total, d)
    return jnp.where(d > total - 1 - HALO, d - total, d)


def factors(offset, within, fall, radius):
    u = offset - within
    env = jnp.where(jnp.abs(offset) <= radius, jnp.exp2(fall * (u * u)), 0.0)
    s = u * (1.0 / HALO)
    out = [env]
    for _ in range(DEG):
        out.append(out[-1] * s)
    return out


def split(v):
    hi = v.astype(bf16)
    return hi, (v - hi.astype(f32)).astype(bf16)


def nt(a, b):
    return lax.dot_general(a, b, (((1,), (1,)), ((), ())), preferred_element_type=f32)


class Sizes:
    def __init__(self, n_gx, n_gy, n_gz, pair_dev):
        self.n_gx, self.n_gy, self.n_gz = n_gx, n_gy, n_gz
        self.nx, self.ny, self.nz = CX * n_gx, CY * n_gy, CZ * n_gz
        self.nky, self.nkz = self.ny // n_gx, self.nz // (n_gy * n_gz)
        self.pair_dev = pair_dev
        self.per = LANES // pair_dev
        self.groups = n_gx // self.per
        self.wide = max(self.nx, LANES)
        self.kys = self.wide // self.nx
        self.blocks = self.nky // self.kys
        self.cols = 2 * self.nkz * n_gy
        self.rows = self.nky * self.nx


def source_z(z, gz, r):
    step = jnp.where(gz < z.n_gz // 2, r, z.n_gz - r)
    return lax.rem(gz + step, z.n_gz)


def kz_of(z, gy, gz):
    starts = []
    for dy in range(z.n_gy):
        block = lax.rem(gy + dy, z.n_gy) * z.n_gz + gz
        starts.append(iota_f((z.nkz, 1), 0) + (block * z.nkz).astype(f32))
    return jnp.concatenate(starts, axis=0)


def paired(z, a, b):
    n = z.nkz
    out = []
    for dy in range(z.n_gy):
        out += [a[dy * n : (dy + 1) * n], b[dy * n : (dy + 1) * n]]
    return jnp.concatenate(out, axis=0)


def z_tables(z, place, ztab):
    gx, gy, gz = place
    kz = kz_of(z, gy, gz)
    col = lax.broadcasted_iota(jnp.int32, (1, CZW), 1)
    cell = jnp.where(col < CZ + HALO, col, col - CZW).astype(f32)
    c0, s0 = cos_sin(kz * cell * (1.0 / z.nz))
    for r in range(z.n_gz):
        source = source_z(z, gz, r).astype(f32)
        ca, sa = cos_sin(kz * source * (1.0 / z.n_gz))
        c = c0 * ca - s0 * sa
        s = s0 * ca + c0 * sa
        hi, lo = split(paired(z, c, -s))
        ztab[r] = jnp.concatenate([hi, hi, lo], axis=1)


def y_table(z, place, ytab):
    gx, gy, gz = place
    row = lax.broadcasted_iota(jnp.int32, (2 * z.nky, 1), 0)
    ky = (row // (2 * z.kys) * z.kys + row % z.kys + gx * z.nky).astype(f32)
    y = iota_f((1, CYW), 1) + ((gy * CY).astype(f32) - HALO)
    c, s = cos_sin(ky * y * (1.0 / z.ny))
    hi, lo = split(jnp.where(row % (2 * z.kys) < z.kys, c, -s))
    ytab[...] = jnp.concatenate([hi, hi, lo], axis=1)


def put3(ref, rows, k, hi, lo, order):
    for n, which in enumerate(order):
        ref[rows, n * DEPTH + k * LANES : n * DEPTH + (k + 1) * LANES] = lo if which else hi


def stack3(ref, k, v):
    hi, lo = split(v)
    n = v.shape[0]
    lanes = slice(k * LANES, (k + 1) * LANES)
    ref[:n, lanes] = hi
    ref[n : 2 * n, lanes] = lo
    ref[2 * n :, lanes] = hi


def chunk_work(z, place, r, prm, s, after=None):
    gx, gy, gz = place
    row = lambda a: prm[a : a + 1, :]
    cx, cy, cz, ox, oy, oz, rate, radius = [row(COEFS + n) for n in range(8)]
    fall = rate * (-1.0 / math.log(2.0))
    nx = z.nx

    fy = factors(iota_f((CYW, LANES), 0) + ((gy * CY).astype(f32) - HALO) - cy, oy, fall, radius)
    for j in range(SIDE):
        s.fy[j] = fy[j]
        stack3(s.yw, j, fy[j])
    part = jnp.dot(s.ytab[...], s.yw[...], preferred_element_type=f32)
    for k in range(SIDE):
        for i in range(SIDE):
            v = None
            for j in range(SIDE):
                w = row((i * SIDE + j) * SIDE + k) * part[:, j * LANES : (j + 1) * LANES]
                v = w if v is None else v + w
            for g in range(z.blocks):
                s.h[k * SIDE + i, g] = v[2 * z.kys * g : 2 * z.kys * (g + 1)]

    fx = factors(wrapped(iota_f((nx, LANES), 0), cx, float(z.nx)), ox, fall, radius)
    fxl = factors(
        wrapped(iota_f((CX, LANES), 0) + (gx * CX).astype(f32), cx, float(z.nx)), ox, fall, radius
    )
    for k in range(SIDE):
        for j in range(SIDE):
            v = None
            for i in range(SIDE):
                w = row((i * SIDE + j) * SIDE + k) * fxl[i]
                v = w if v is None else v + w
            s.hd[k * SIDE + j] = v

    cell = lax.broadcasted_iota(jnp.int32, (CZW, LANES), 0)
    cell = jnp.where(cell < CZ + HALO, cell, cell - CZW).astype(f32)
    source = source_z(z, gz, r) * CZ
    fz = factors(cell - (cz - source.astype(f32)), oz, fall, radius)
    for k in range(SIDE):
        s.fe[0, k] = fz[k][CZ + HALO :]
        s.fe[1, k] = fz[k][CZ : CZ + HALO]
        stack3(s.zw, k, fz[k])
    for k in range(SIDE):
        lanes = slice(k * LANES, (k + 1) * LANES)
        v = jnp.dot(s.ztab[r], s.zw[:, lanes], preferred_element_type=f32)
        hi, lo = split(v)
        put3(s.z, slice(0, z.cols), k, hi, lo, (0, 0, 1))

    def cells():
        for x in range(CX):
            for k in range(SIDE):
                v = None
                for j in range(SIDE):
                    w = s.hd[k * SIDE + j, x : x + 1, :] * s.fy[j]
                    v = w if v is None else v + w
                hi, lo = split(v)
                put3(s.d, slice(x * CYW, (x + 1) * CYW), k, hi, lo, (0, 1, 0))
        hi, lo = s.zw[:CZ], s.zw[CZW : CZW + CZ]
        more = nt(s.d[...], jnp.concatenate([hi, hi, lo], axis=1))
        s.dacc[...] = s.dacc[...] + more.reshape(CX, CYW, CZ)

    def edge(which):
        for x in range(0, CX, 2):
            for j in range(SIDE):
                both = []
                for xx in (x, x + 1):
                    v = None
                    for k in range(SIDE):
                        w = s.hd[k * SIDE + j, xx : xx + 1, :] * s.fe[which, k]
                        v = w if v is None else v + w
                    both.append(v)
                hi, lo = split(jnp.concatenate(both, axis=0))
                put3(s.te, slice(x * HALO, (x + 2) * HALO), j, hi, lo, (0, 0, 1))
        hi, lo = s.yw[:CYW], s.yw[CYW : 2 * CYW]
        more = nt(jnp.concatenate([hi, lo, hi], axis=1), s.te[...])
        s.eacc[which] = s.eacc[which] + more

    def build(g):
        for m in range(2):
            for kk in range(z.kys):
                o = m * z.wide + kk * nx
                for k in range(SIDE):
                    v = None
                    for i in range(SIDE):
                        q = m * z.kys + kk
                        w = s.h[k * SIDE + i, g, q : q + 1, :] * fx[i]
                        v = w if v is None else v + w
                    hi, lo = split(v)
                    put3(s.t[g % TS], slice(o, o + nx), k, hi, lo, (0, 1, 0))

    def product(g):
        rows = slice(2 * z.wide * g, 2 * z.wide * (g + 1))
        s.acc[rows] = s.acc[rows] + nt(s.t[g % TS][...], s.z[...])

    near = jnp.where(gz < z.n_gz // 2, 0, 1)
    if after is not None:
        edge(1 - near)
        add_edges(s.dacc, s.eacc)
    build(0)
    for g in range(1, z.blocks):
        build(g)
        product(g - 1)
    product(z.blocks - 1)
    if after is not None:
        return
    pl.when(r == 0)(cells)
    pl.when(r == 1)(lambda: edge(near))
    if z.groups > 1:
        pl.when(r == z.n_gz - 1)(lambda: edge(1 - near))


class Scratch:
    pass


def params_of(z, cells, offs, e_index, r_index, exponents, pm):
    n = z.pair_dev
    pm[...] = jnp.zeros_like(pm)
    radius = (HALO - r_index[...]).astype(f32)
    chosen = None
    for e in range(exponents.shape[0]):
        w = jnp.where(e_index[...] == e, exponents[e], 0.0)
        chosen = w if chosen is None else chosen + w
    pm[0:3, :n] = cells[...].astype(f32)
    pm[3:6, :n] = offs[...]
    pm[6:7, :n] = chosen / (radius * radius)
    pm[7:8, :n] = radius


def coefficients(z, basis, blocks):
    bh, bl = split(basis[...])
    ph, pb = split(blocks[...])
    ph = jnp.concatenate([ph] * FOLD, axis=0)
    pb = jnp.concatenate([pb] * FOLD, axis=0)
    both = nt(bh, ph) + (nt(bh, pb) + nt(bl, ph))
    lane = lax.broadcasted_iota(jnp.int32, (TOP, FOLD * z.pair_dev), 1) // z.pair_dev
    v = both[:TOP]
    for g in range(1, FOLD):
        v = jnp.where(lane == g, both[g * TOP : (g + 1) * TOP], v)
    return v


def unpack(z, blocks, prm):
    owner = lax.broadcasted_iota(jnp.int32, (TOP, LANES), 1) // z.pair_dev
    for g in range(FOLD):
        v = None
        for d, block in enumerate(blocks):
            shift = (d - g) % FOLD * z.pair_dev
            w = block[:TOP]
            w = pltpu.roll(w, shift, 1) if shift else w
            v = w if v is None else jnp.where(owner == d, w, v)
        prm[g * TOP : (g + 1) * TOP] = v
    v = None
    for d, block in enumerate(blocks):
        w = block[TOP:]
        w = pltpu.roll(w, d * z.pair_dev, 1) if d else w
        v = w if v is None else jnp.where(owner[:8] == d, w, v)
    prm[COEFS : COEFS + 8] = v


def swapped(z, b):
    lane = lax.broadcasted_iota(jnp.int32, (b.shape[0], LANES), 1)
    first = lane % (2 * z.nkz) < z.nkz
    out = []
    for c in range(z.cols // LANES):
        w = b[:, c * LANES : (c + 1) * LANES]
        down = pltpu.roll(w, LANES - z.nkz, 1)
        up = down if 2 * z.nkz == LANES else pltpu.roll(w, z.nkz, 1)
        out.append(jnp.where(first, down, -up))
    return jnp.concatenate(out, axis=1)


def kernel(
    z, basis_hbm, blocks_hbm, cells_hbm, offs_hbm, ei_hbm, ri_hbm, ex_hbm, xt_hbm,
    own, got, dacc, edges,
    basis, blocks, cells, offs, e_index, r_index, exponents, xt, pm, prm, cols, give,
    h, hd, fy, fe, acc, eacc,
    ready, in_sem, send_z, recv_z, send_c, recv_c, send_e, recv_e, send_d, recv_d,
):
    n_gx, n_gy, n_gz = z.n_gx, z.n_gy, z.n_gz
    gx, gy, gz = (lax.axis_index(a) for a in ("gx", "gy", "gz"))
    place = gx, gy, gz
    mesh_type = pl.DeviceIdType.MESH

    def along_z(r):
        return gx, gy, lax.rem(gz + n_gz - r, n_gz)

    def along_x(dx):
        return lax.rem(gx + n_gx - dx, n_gx), gy, gz

    def along_y(dy):
        return gx, lax.rem(gy + n_gy + dy, n_gy), gz

    barrier = pltpu.get_barrier_semaphore()
    for r in range(1, n_gz):

        @pl.when(r > gz)
        def _(r=r):
            pl.semaphore_signal(barrier, inc=1, device_id=along_z(r), device_id_type=mesh_type)

    def greet(dx, carry):
        pl.semaphore_signal(barrier, inc=1, device_id=along_x(dx), device_id_type=mesh_type)
        return carry

    lax.fori_loop(1, n_gx, greet, 0)
    for dy in range(1, n_gy):
        pl.semaphore_signal(barrier, inc=1, device_id=along_y(dy), device_id_type=mesh_type)

    pairs = [
        (blocks_hbm, blocks), (basis_hbm, basis), (cells_hbm, cells), (offs_hbm, offs),
        (ei_hbm, e_index), (ri_hbm, r_index), (ex_hbm, exponents), (xt_hbm, xt),
    ]
    loads = [
        pltpu.make_async_copy(a, b, in_sem.at[n]) for n, (a, b) in enumerate(pairs)
    ]
    for c in loads:
        c.start()
    with jax.named_scope("load_wait"):
        for c in loads[:-1]:
            c.wait()
    with jax.named_scope("coefs"):
        params_of(z, cells, offs, e_index, r_index, exponents, pm)
        cols[0, 0, :TOP] = coefficients(z, basis, blocks)
        cols[0, 0, TOP:] = pm[...]

    def body(ytab, ztab, t0, t1, t2, t3, zs, d, zw, yw, te):
        s = Scratch()
        s.ytab, s.ztab, s.t, s.z = ytab, ztab, (t0, t1, t2, t3), zs
        s.d, s.zw, s.yw, s.te = d, zw, yw, te
        s.h, s.hd, s.fy, s.fe = h, hd, fy, fe
        s.acc, s.dacc, s.eacc = acc, dacc, eacc
        with jax.named_scope("clear"):
            for ref in (acc, dacc, eacc):
                ref[...] = jnp.zeros_like(ref)
        with jax.named_scope("barrier_wait"):
            pl.semaphore_wait(barrier, n_gx + n_gy - 2 + gz)

        def copy_z(q):
            target = along_z(q)
            slot = jnp.where(target[2] < n_gz // 2, q, n_gz - q)
            return pltpu.make_async_remote_copy(
                src_ref=cols.at[0, 0],
                dst_ref=cols.at[slot, 0],
                send_sem=send_z.at[q],
                recv_sem=recv_z.at[slot],
                device_id=target,
                device_id_type=mesh_type,
            )

        def wait_z(r):
            with jax.named_scope(f"z_wait{r}"):
                pltpu.make_async_remote_copy(
                    src_ref=cols.at[0, 0],
                    dst_ref=cols.at[r, 0],
                    send_sem=send_z.at[r],
                    recv_sem=recv_z.at[r],
                    device_id=along_z(r),
                    device_id_type=mesh_type,
                ).wait_recv()
            forward(r)

        def copy_c(r, dx):
            return pltpu.make_async_remote_copy(
                src_ref=cols.at[r, 0],
                dst_ref=cols.at[r, dx],
                send_sem=send_c.at[r * n_gx + dx],
                recv_sem=recv_c.at[r * n_gx + dx],
                device_id=along_x(dx),
                device_id_type=mesh_type,
            )

        def forward(r):
            def one(dx, carry):
                copy_c(r, dx).start()
                return carry

            lax.fori_loop(1, n_gx, one, 0)

        for r in range(1, n_gz):

            @pl.when(r <= gz)
            def _(r=r):
                pl.semaphore_signal(
                    ready.at[n_gz - r], inc=1, device_id=along_z(r), device_id_type=mesh_type
                )
                copy_z(r).start()

        forward(0)
        with jax.named_scope("tables"):
            y_table(z, place, ytab)
            z_tables(z, place, ztab)
        def send_up(distance):
            @pl.when(gz + distance < n_gz)
            def _():
                pl.semaphore_wait(ready.at[n_gz - distance], 1)
                copy_z(n_gz - distance).start()

        send_up(1)
        wait_z(1)
        for distance in range(2, n_gz - 1):
            send_up(distance)

        def arrive(r, g):
            with jax.named_scope("x_wait"):
                for d in range(z.per):
                    dx = g * z.per + d

                    @pl.when(dx > 0)
                    def _(dx=dx):
                        copy_c(r, dx).wait_recv()

            unpack(z, [cols[r, g * z.per + d] for d in range(z.per)], prm)

        lower = gz < n_gz // 2

        def second():
            send_up(n_gz - 1)
            for r in range(2, n_gz - 1):
                wait_z(r)

            @pl.when(lower)
            def _():
                wait_z(n_gz - 1)

        def third():
            @pl.when(jnp.logical_not(lower))
            def _():
                wait_z(n_gz - 1)

        def chunk(c, carry):
            r, g = c // z.groups, c % z.groups
            pl.when(c == z.groups)(second)
            pl.when(c == 2 * z.groups)(third)
            arrive(r, g)
            with jax.named_scope("chunk"):
                chunk_work(z, place, r, prm, s)
            return carry

        lax.fori_loop(0, n_gz * z.groups - 1, chunk, 0)

        def copy_d(which):
            return pltpu.make_async_remote_copy(
                src_ref=dacc.at[:, pl.ds(which * (CY + HALO), HALO), :],
                dst_ref=edges.at[which],
                send_sem=send_d.at[which],
                recv_sem=recv_d.at[which],
                device_id=along_y(2 * which - 1),
                device_id_type=mesh_type,
            )

        def copy_e(dy, g):
            rows = pl.ds(g * z.wide, z.wide)
            return pltpu.make_async_remote_copy(
                src_ref=give.at[dy - 1, rows],
                dst_ref=got.at[dy - 1, rows],
                send_sem=send_e.at[dy * z.blocks + g],
                recv_sem=recv_e.at[dy * z.blocks + g],
                device_id=along_y(dy),
                device_id_type=mesh_type,
            )

        loads[-1].wait()

        def x_transform(g):
            v = acc[2 * z.wide * g : 2 * z.wide * (g + 1)]
            hi, lo = split(v)
            for kk in range(z.kys):
                parts = [
                    w[m * z.wide + kk * z.nx : m * z.wide + (kk + 1) * z.nx]
                    for w in (hi, lo, hi)
                    for m in range(2)
                ]
                q = jnp.dot(xt[...], jnp.concatenate(parts, axis=0), preferred_element_type=f32)
                out = q[: z.nx] + swapped(z, q[z.nx :])
                start = g * z.wide + kk * z.nx
                rows = slice(start, start + z.nx)
                own[rows] = out[:, : 2 * z.nkz]
                for dy in range(1, n_gy):
                    give[dy - 1, rows] = out[:, 2 * z.nkz * dy : 2 * z.nkz * (dy + 1)]

        arrive(n_gz - 1, z.groups - 1)
        with jax.named_scope("last"):
            chunk_work(z, place, n_gz - 1, prm, s, x_transform)
        for which in range(2):
            copy_d(which).start()
        for g in range(z.blocks):
            x_transform(g)
        for g in range(z.blocks):
            for dy in range(1, n_gy):
                copy_e(dy, g).start()
        with jax.named_scope("drain"):
            for r in range(1, n_gz):
                copy_z(r).wait_send()

        def drain(c, carry):
            @pl.when(c % n_gx > 0)
            def _():
                copy_c(c // n_gx, c % n_gx).wait_send()

            return carry

        lax.fori_loop(0, n_gz * n_gx, drain, 0)
        with jax.named_scope("exchange_wait"):
            for which in range(2):
                copy_d(which).wait()
            for g in range(z.blocks):
                for dy in range(1, n_gy):
                    copy_e(dy, g).wait()

    pl.run_scoped(
        body,
        pltpu.VMEM((2 * z.nky, 3 * CYW), bf16),
        pltpu.VMEM((n_gz, z.cols, 3 * CZW), bf16),
        *[pltpu.VMEM((2 * z.wide, 3 * DEPTH), bf16)] * TS,
        pltpu.VMEM((z.cols, 3 * DEPTH), bf16),
        pltpu.VMEM((CX * CYW, 3 * DEPTH), bf16),
        pltpu.VMEM((3 * CZW, DEPTH), bf16),
        pltpu.VMEM((3 * CYW, DEPTH), bf16),
        pltpu.VMEM((CX * HALO, 3 * DEPTH), bf16),
    )


def add_edges(dacc, eacc):
    lane = lax.broadcasted_iota(jnp.int32, (CYW, LANES), 1)
    pad = jnp.zeros((CYW, LANES - CX * HALO), f32)
    for which, start in ((0, LANES - HALO), (1, 0)):
        e = jnp.concatenate([eacc[which], pad], axis=1)
        mask = (lane >= start) & (lane < start + HALO)
        for x in range(CX):
            v = pltpu.roll(e, (start - x * HALO) % LANES, 1)
            dacc[x] = dacc[x] + jnp.where(mask, v, 0.0)


def finish(z, own, got, dacc, edges, dens_ref, spec_ref):
    total = own[...]
    for dy in range(1, z.n_gy):
        total = total + got[dy - 1]
    spec_ref[0] = total[:, : z.nkz]
    spec_ref[1] = total[:, z.nkz :]
    dens_ref[...] = dacc[:, HALO : HALO + CY]
    dens_ref[:, CY - HALO :] = dens_ref[:, CY - HALO :] + edges[0]
    dens_ref[:, :HALO] = dens_ref[:, :HALO] + edges[1]


def x_table(z):
    idx = np.arange(z.nx)
    angle = (idx[:, None] * idx[None, :] % z.nx) * (2.0 * math.pi / z.nx)
    c, s = np.cos(angle), np.sin(angle)
    full = np.block([[c, s], [s, -c]]) / math.sqrt(z.nx * z.ny * z.nz)
    full = full.astype(np.float32)
    hi = full.astype(ml_dtypes.bfloat16)
    lo = (full - hi.astype(np.float32)).astype(ml_dtypes.bfloat16)
    return np.concatenate([hi, hi, lo], axis=1)


def shards(
    pair_blocks, basis_map, pair_cells, pair_offsets, exponent_index, radius_index, exponents
):
    n_gx, n_gy, n_gz = (lax.axis_size(a) for a in ("gx", "gy", "gz"))
    pair_dev = pair_blocks.shape[1]
    z = Sizes(n_gx, n_gy, n_gz, pair_dev)
    assert FOLD * pair_dev == LANES and n_gx % z.per == 0 and n_gz >= 3 and n_gy >= 2
    in_vmem = pl.BlockSpec(memory_space=pltpu.VMEM)
    in_hbm = pl.BlockSpec(memory_space=pltpu.HBM)
    basis = basis_map.T
    blocks = pair_blocks.T
    xt = jnp.asarray(x_table(z))
    ei, ri = exponent_index.reshape(1, -1), radius_index.reshape(1, -1)
    dma = pltpu.SemaphoreType.DMA
    own, got, dacc, edges = pl.pallas_call(
        functools.partial(kernel, z),
        out_shape=[
            jax.ShapeDtypeStruct((z.rows, 2 * z.nkz), f32),
            jax.ShapeDtypeStruct((n_gy - 1, z.rows, 2 * z.nkz), f32),
            jax.ShapeDtypeStruct((CX, CYW, CZ), f32),
            jax.ShapeDtypeStruct((2, CX, HALO, CZ), f32),
        ],
        in_specs=[in_hbm] * 8,
        out_specs=[in_vmem] * 4,
        scratch_shapes=[
            pltpu.VMEM(basis.shape, f32),
            pltpu.VMEM(blocks.shape, f32),
            pltpu.VMEM(pair_cells.shape, jnp.int32),
            pltpu.VMEM(pair_offsets.shape, f32),
            pltpu.VMEM(ei.shape, jnp.int32),
            pltpu.VMEM(ri.shape, jnp.int32),
            pltpu.SMEM(exponents.shape, f32),
            pltpu.VMEM(xt.shape, bf16),
            pltpu.VMEM((8, LANES), f32),
            pltpu.VMEM((COEFS + 8, LANES), f32),
            pltpu.VMEM((n_gz, n_gx, BLOCK_ROWS, LANES), f32),
            pltpu.VMEM((n_gy - 1, z.rows, 2 * z.nkz), f32),
            pltpu.VMEM((SIDE * SIDE, z.blocks, 2 * z.kys, LANES), f32),
            pltpu.VMEM((SIDE * SIDE, CX, LANES), f32),
            pltpu.VMEM((SIDE, CYW, LANES), f32),
            pltpu.VMEM((2, SIDE, HALO, LANES), f32),
            pltpu.VMEM((2 * z.rows, z.cols), f32),
            pltpu.VMEM((2, CYW, CX * HALO), f32),
            pltpu.SemaphoreType.REGULAR((n_gz,)),
            dma((8,)),
            dma((n_gz,)),
            dma((n_gz,)),
            dma((n_gz * n_gx,)),
            dma((n_gz * n_gx,)),
            dma((n_gy * z.blocks,)),
            dma((n_gy * z.blocks,)),
            dma((2,)),
            dma((2,)),
        ],
        compiler_params=pltpu.CompilerParams(
            collective_id=0, has_side_effects=True, vmem_limit_bytes=VMEM_LIMIT
        ),
    )(
        *(
            pltpu.with_memory_space_constraint(a, pltpu.HBM)
            for a in (basis, blocks, pair_cells, pair_offsets, ei, ri, exponents, xt)
        )
    )
    dens, spec = pl.pallas_call(
        functools.partial(finish, z),
        out_shape=[
            jax.ShapeDtypeStruct((CX, CY, CZ), f32),
            jax.ShapeDtypeStruct((2, z.rows, z.nkz), f32),
        ],
        in_specs=[in_vmem] * 4,
        out_specs=[in_vmem] * 2,
        compiler_params=pltpu.CompilerParams(vmem_limit_bytes=VMEM_LIMIT),
    )(own, got, dacc, edges)
    return dens, spec.reshape(2, z.nky, z.nx, z.nkz).transpose(0, 3, 1, 2)


def solution(mesh):
    placed = (
        P(None, ("gx", "gy", "gz")),
        P(),
        P(None, ("gx", "gy", "gz")),
        P(None, ("gx", "gy", "gz")),
        P(("gx", "gy", "gz")),
        P(("gx", "gy", "gz")),
        P(),
    )
    return jax.shard_map(
        shards,
        mesh=mesh,
        in_specs=placed,
        out_specs=(P("gx", "gy", "gz"), P(None, ("gy", "gz"), "gx", None)),
        check_vma=False,
    )
```

```python
import functools
import math

import jax
import jax.numpy as jnp
import ml_dtypes
import numpy as np
from jax import lax
from jax.experimental import pallas as pl
from jax.experimental.pallas import tpu as pltpu
from jax.sharding import PartitionSpec as P

DEG = 3
HALO = 8
CX = 8
CY = 32
CZ = 128
SIDE = DEG + 1
LANES = 128
VMEM_LIMIT = 40 << 20
COEFS = SIDE**3
FOLD = 4
TOP = COEFS // FOLD
BLOCK_ROWS = TOP + 8
CYW = CY + 2 * HALO
CZW = CZ + 2 * HALO
TS = 4
DEPTH = SIDE * LANES

f32 = jnp.float32
bf16 = jnp.bfloat16


def iota_f(shape, dim):
    return lax.broadcasted_iota(jnp.int32, shape, dim).astype(f32)


def cos_sin(turns):
    r = turns - jnp.floor(turns + 0.5)
    t = r * math.pi
    t2 = t * t
    s = t * _poly(t2, [(-1) ** n / math.factorial(2 * n + 1) for n in range(7)])
    c = _poly(t2, [(-1) ** n / math.factorial(2 * n) for n in range(8)])
    return 1.0 - 2.0 * s * s, 2.0 * s * c


def _poly(x, coefs):
    out = jnp.full_like(x, coefs[-1])
    for a in reversed(coefs[:-1]):
        out = out * x + a
    return out


def wrapped(cells, centre, total):
    d = cells - centre
    d = jnp.where(d < -HALO, d + total, d)
    return jnp.where(d > total - 1 - HALO, d - total, d)


def factors(offset, within, fall, radius):
    u = offset - within
    env = jnp.where(jnp.abs(offset) <= radius, jnp.exp2(fall * (u * u)), 0.0)
    s = u * (1.0 / HALO)
    out = [env]
    for _ in range(DEG):
        out.append(out[-1] * s)
    return out


def split(v):
    hi = v.astype(bf16)
    return hi, (v - hi.astype(f32)).astype(bf16)


def nt(a, b):
    return lax.dot_general(a, b, (((1,), (1,)), ((), ())), preferred_element_type=f32)


class Sizes:
    def __init__(self, n_gx, n_gy, n_gz, pair_dev):
        self.n_gx, self.n_gy, self.n_gz = n_gx, n_gy, n_gz
        self.nx, self.ny, self.nz = CX * n_gx, CY * n_gy, CZ * n_gz
        self.nky, self.nkz = self.ny // n_gx, self.nz // (n_gy * n_gz)
        self.pair_dev = pair_dev
        self.per = LANES // pair_dev
        self.groups = n_gx // self.per
        self.wide = max(self.nx, LANES)
        self.kys = self.wide // self.nx
        self.blocks = self.nky // self.kys
        self.cols = 2 * self.nkz * n_gy
        self.rows = self.nky * self.nx


def source_z(z, gz, r):
    step = jnp.where(gz < z.n_gz // 2, r, z.n_gz - r)
    return lax.rem(gz + step, z.n_gz)


def kz_of(z, gy, gz):
    starts = []
    for dy in range(z.n_gy):
        block = lax.rem(gy + dy, z.n_gy) * z.n_gz + gz
        starts.append(iota_f((z.nkz, 1), 0) + (block * z.nkz).astype(f32))
    return jnp.concatenate(starts, axis=0)


def paired(z, a, b):
    n = z.nkz
    out = []
    for dy in range(z.n_gy):
        out += [a[dy * n : (dy + 1) * n], b[dy * n : (dy + 1) * n]]
    return jnp.concatenate(out, axis=0)


def z_tables(z, place, ztab):
    gx, gy, gz = place
    kz = kz_of(z, gy, gz)
    col = lax.broadcasted_iota(jnp.int32, (1, CZW), 1)
    cell = jnp.where(col < CZ + HALO, col, col - CZW).astype(f32)
    c0, s0 = cos_sin(kz * cell * (1.0 / z.nz))
    for r in range(z.n_gz):
        source = source_z(z, gz, r).astype(f32)
        ca, sa = cos_sin(kz * source * (1.0 / z.n_gz))
        c = c0 * ca - s0 * sa
        s = s0 * ca + c0 * sa
        hi, lo = split(paired(z, c, -s))
        ztab[r] = jnp.concatenate([hi, hi, lo], axis=1)


def y_table(z, place, ytab):
    gx, gy, gz = place
    row = lax.broadcasted_iota(jnp.int32, (2 * z.nky, 1), 0)
    ky = (row // (2 * z.kys) * z.kys + row % z.kys + gx * z.nky).astype(f32)
    y = iota_f((1, CYW), 1) + ((gy * CY).astype(f32) - HALO)
    c, s = cos_sin(ky * y * (1.0 / z.ny))
    hi, lo = split(jnp.where(row % (2 * z.kys) < z.kys, c, -s))
    ytab[...] = jnp.concatenate([hi, hi, lo], axis=1)


def put3(ref, rows, k, hi, lo, order):
    for n, which in enumerate(order):
        ref[rows, n * DEPTH + k * LANES : n * DEPTH + (k + 1) * LANES] = lo if which else hi


def stack3(ref, k, v):
    hi, lo = split(v)
    n = v.shape[0]
    lanes = slice(k * LANES, (k + 1) * LANES)
    ref[:n, lanes] = hi
    ref[n : 2 * n, lanes] = lo
    ref[2 * n :, lanes] = hi


def chunk_work(z, place, r, prm, s, after=None):
    gx, gy, gz = place
    row = lambda a: prm[a : a + 1, :]
    cx, cy, cz, ox, oy, oz, rate, radius = [row(COEFS + n) for n in range(8)]
    fall = rate * (-1.0 / math.log(2.0))
    nx = z.nx

    fy = factors(iota_f((CYW, LANES), 0) + ((gy * CY).astype(f32) - HALO) - cy, oy, fall, radius)
    for j in range(SIDE):
        s.fy[j] = fy[j]
        stack3(s.yw, j, fy[j])
    part = jnp.dot(s.ytab[...], s.yw[...], preferred_element_type=f32)
    for k in range(SIDE):
        for i in range(SIDE):
            v = None
            for j in range(SIDE):
                w = row((i * SIDE + j) * SIDE + k) * part[:, j * LANES : (j + 1) * LANES]
                v = w if v is None else v + w
            for g in range(z.blocks):
                s.h[k * SIDE + i, g] = v[2 * z.kys * g : 2 * z.kys * (g + 1)]

    fx = factors(wrapped(iota_f((nx, LANES), 0), cx, float(z.nx)), ox, fall, radius)
    fxl = factors(
        wrapped(iota_f((CX, LANES), 0) + (gx * CX).astype(f32), cx, float(z.nx)), ox, fall, radius
    )
    for k in range(SIDE):
        for j in range(SIDE):
            v = None
            for i in range(SIDE):
                w = row((i * SIDE + j) * SIDE + k) * fxl[i]
                v = w if v is None else v + w
            s.hd[k * SIDE + j] = v

    cell = lax.broadcasted_iota(jnp.int32, (CZW, LANES), 0)
    cell = jnp.where(cell < CZ + HALO, cell, cell - CZW).astype(f32)
    source = source_z(z, gz, r) * CZ
    fz = factors(cell - (cz - source.astype(f32)), oz, fall, radius)
    for k in range(SIDE):
        s.fe[0, k] = fz[k][CZ + HALO :]
        s.fe[1, k] = fz[k][CZ : CZ + HALO]
        stack3(s.zw, k, fz[k])
    for k in range(SIDE):
        lanes = slice(k * LANES, (k + 1) * LANES)
        v = jnp.dot(s.ztab[r], s.zw[:, lanes], preferred_element_type=f32)
        hi, lo = split(v)
        put3(s.z, slice(0, z.cols), k, hi, lo, (0, 0, 1))

    def build(g):
        for m in range(2):
            for kk in range(z.kys):
                o = m * z.wide + kk * nx
                for k in range(SIDE):
                    v = None
                    for i in range(SIDE):
                        q = m * z.kys + kk
                        w = s.h[k * SIDE + i, g, q : q + 1, :] * fx[i]
                        v = w if v is None else v + w
                    hi, lo = split(v)
                    put3(s.t[g % TS], slice(o, o + nx), k, hi, lo, (0, 1, 0))

    def product(g):
        rows = slice(2 * z.wide * g, 2 * z.wide * (g + 1))
        s.acc[rows] = s.acc[rows] + nt(s.t[g % TS][...], s.z[...])

    if after is not None:
        density_work(z, place, r, s)
        add_edges(s.dacc, s.eacc)
    build(0)
    for g in range(1, z.blocks):
        build(g)
        product(g - 1)
    product(z.blocks - 1)


def density_work(z, place, r, s):
    near = jnp.where(place[2] < z.n_gz // 2, 0, 1)

    def cells():
        for x in range(CX):
            for k in range(SIDE):
                v = None
                for j in range(SIDE):
                    w = s.hd[k * SIDE + j, x : x + 1, :] * s.fy[j]
                    v = w if v is None else v + w
                hi, lo = split(v)
                put3(s.d, slice(x * CYW, (x + 1) * CYW), k, hi, lo, (0, 1, 0))
        hi, lo = s.zw[:CZ], s.zw[CZW : CZW + CZ]
        more = nt(s.d[...], jnp.concatenate([hi, hi, lo], axis=1))
        s.dacc[...] = s.dacc[...] + more.reshape(CX, CYW, CZ)

    def edge(which):
        for x in range(0, CX, 2):
            for j in range(SIDE):
                both = []
                for xx in (x, x + 1):
                    v = None
                    for k in range(SIDE):
                        w = s.hd[k * SIDE + j, xx : xx + 1, :] * s.fe[which, k]
                        v = w if v is None else v + w
                    both.append(v)
                hi, lo = split(jnp.concatenate(both, axis=0))
                put3(s.te, slice(x * HALO, (x + 2) * HALO), j, hi, lo, (0, 0, 1))
        hi, lo = s.yw[:CYW], s.yw[CYW : 2 * CYW]
        more = nt(jnp.concatenate([hi, lo, hi], axis=1), s.te[...])
        s.eacc[which] = s.eacc[which] + more

    if isinstance(r, int):
        edge(1 - near)
        return
    pl.when(r == 0)(cells)
    pl.when(r == 1)(lambda: edge(near))
    if z.groups > 1:
        pl.when(r == z.n_gz - 1)(lambda: edge(1 - near))


class Scratch:
    pass


def params_of(z, cells, offs, e_index, r_index, exponents, pm):
    n = z.pair_dev
    pm[...] = jnp.zeros_like(pm)
    radius = (HALO - r_index[...]).astype(f32)
    chosen = None
    for e in range(exponents.shape[0]):
        w = jnp.where(e_index[...] == e, exponents[e], 0.0)
        chosen = w if chosen is None else chosen + w
    pm[0:3, :n] = cells[...].astype(f32)
    pm[3:6, :n] = offs[...]
    pm[6:7, :n] = chosen / (radius * radius)
    pm[7:8, :n] = radius


def coefficients(z, basis, blocks):
    bh, bl = split(basis[...])
    ph, pb = split(blocks[...])
    ph = jnp.concatenate([ph] * FOLD, axis=0)
    pb = jnp.concatenate([pb] * FOLD, axis=0)
    both = nt(bh, ph) + (nt(bh, pb) + nt(bl, ph))
    lane = lax.broadcasted_iota(jnp.int32, (TOP, FOLD * z.pair_dev), 1) // z.pair_dev
    v = both[:TOP]
    for g in range(1, FOLD):
        v = jnp.where(lane == g, both[g * TOP : (g + 1) * TOP], v)
    return v


def unpack(z, blocks, prm):
    owner = lax.broadcasted_iota(jnp.int32, (TOP, LANES), 1) // z.pair_dev
    for g in range(FOLD):
        v = None
        for d, block in enumerate(blocks):
            shift = (d - g) % FOLD * z.pair_dev
            w = block[:TOP]
            w = pltpu.roll(w, shift, 1) if shift else w
            v = w if v is None else jnp.where(owner == d, w, v)
        prm[g * TOP : (g + 1) * TOP] = v
    v = None
    for d, block in enumerate(blocks):
        w = block[TOP:]
        w = pltpu.roll(w, d * z.pair_dev, 1) if d else w
        v = w if v is None else jnp.where(owner[:8] == d, w, v)
    prm[COEFS : COEFS + 8] = v


def swapped(z, b):
    lane = lax.broadcasted_iota(jnp.int32, (b.shape[0], LANES), 1)
    first = lane % (2 * z.nkz) < z.nkz
    out = []
    for c in range(z.cols // LANES):
        w = b[:, c * LANES : (c + 1) * LANES]
        down = pltpu.roll(w, LANES - z.nkz, 1)
        up = down if 2 * z.nkz == LANES else pltpu.roll(w, z.nkz, 1)
        out.append(jnp.where(first, down, -up))
    return jnp.concatenate(out, axis=1)


def kernel(
    z, basis_hbm, blocks_hbm, cells_hbm, offs_hbm, ei_hbm, ri_hbm, ex_hbm, xt_hbm,
    own, got, dacc, edges,
    basis, blocks, cells, offs, e_index, r_index, exponents, xt, pm, prm, cols, give,
    h, hd, fy, fe, acc, eacc,
    ready, in_sem, recv_z, recv_c, recv_e, recv_d,
):
    n_gx, n_gy, n_gz = z.n_gx, z.n_gy, z.n_gz
    gx, gy, gz = (lax.axis_index(a) for a in ("gx", "gy", "gz"))
    place = gx, gy, gz
    mesh_type = pl.DeviceIdType.MESH

    def along_z(r):
        return gx, gy, lax.rem(gz + n_gz - r, n_gz)

    def along_x(dx):
        return lax.rem(gx + n_gx - dx, n_gx), gy, gz

    def along_y(dy):
        return gx, lax.rem(gy + n_gy + dy, n_gy), gz

    barrier = pltpu.get_barrier_semaphore()
    for r in range(1, n_gz):

        @pl.when(r > gz)
        def _(r=r):
            pl.semaphore_signal(barrier, inc=1, device_id=along_z(r), device_id_type=mesh_type)

    def greet(dx, carry):
        pl.semaphore_signal(barrier, inc=1, device_id=along_x(dx), device_id_type=mesh_type)
        return carry

    lax.fori_loop(1, n_gx, greet, 0)
    for dy in range(1, n_gy):
        pl.semaphore_signal(barrier, inc=1, device_id=along_y(dy), device_id_type=mesh_type)

    pairs = [
        (blocks_hbm, blocks), (basis_hbm, basis), (cells_hbm, cells), (offs_hbm, offs),
        (ei_hbm, e_index), (ri_hbm, r_index), (ex_hbm, exponents), (xt_hbm, xt),
    ]
    loads = [
        pltpu.make_async_copy(a, b, in_sem.at[n]) for n, (a, b) in enumerate(pairs)
    ]
    for c in loads:
        c.start()
    with jax.named_scope("load_wait"):
        for c in loads[:-1]:
            c.wait()
    with jax.named_scope("coefs"):
        params_of(z, cells, offs, e_index, r_index, exponents, pm)
        cols[0, 0, :TOP] = coefficients(z, basis, blocks)
        cols[0, 0, TOP:] = pm[...]

    def body(ytab, ztab, t0, t1, t2, t3, zs, d, zw, yw, te):
        s = Scratch()
        s.ytab, s.ztab, s.t, s.z = ytab, ztab, (t0, t1, t2, t3), zs
        s.d, s.zw, s.yw, s.te = d, zw, yw, te
        s.h, s.hd, s.fy, s.fe = h, hd, fy, fe
        s.acc, s.dacc, s.eacc = acc, dacc, eacc
        with jax.named_scope("barrier_wait"):
            pl.semaphore_wait(barrier, n_gx + n_gy - 2 + gz)

        send_z, send_c, send_e, send_d = (in_sem.at[n] for n in range(4))

        def copy_z(q):
            target = along_z(q)
            slot = jnp.where(target[2] < n_gz // 2, q, n_gz - q)
            return pltpu.make_async_remote_copy(
                src_ref=cols.at[0, 0],
                dst_ref=cols.at[slot, 0],
                send_sem=send_z,
                recv_sem=recv_z.at[slot - 1],
                device_id=target,
                device_id_type=mesh_type,
            )

        def wait_z(r):
            with jax.named_scope(f"z_wait{r}"):
                pltpu.make_async_remote_copy(
                    src_ref=cols.at[0, 0],
                    dst_ref=cols.at[r, 0],
                    send_sem=send_z,
                    recv_sem=recv_z.at[r - 1],
                    device_id=along_z(r),
                    device_id_type=mesh_type,
                ).wait_recv()
            forward(r)

        def copy_c(r, dx):
            return pltpu.make_async_remote_copy(
                src_ref=cols.at[r, 0],
                dst_ref=cols.at[r, dx],
                send_sem=send_c,
                recv_sem=recv_c.at[r * z.groups + dx // z.per],
                device_id=along_x(dx),
                device_id_type=mesh_type,
            )

        def forward(r):
            def one(dx, carry):
                copy_c(r, dx).start()
                return carry

            lax.fori_loop(1, n_gx, one, 0)

        for r in range(1, n_gz):

            @pl.when(r <= gz)
            def _(r=r):
                pl.semaphore_signal(
                    ready.at[n_gz - r - 1], inc=1, device_id=along_z(r), device_id_type=mesh_type
                )
                copy_z(r).start()

        forward(0)
        with jax.named_scope("tables"):
            for ref in (acc, dacc, eacc):
                ref[...] = jnp.zeros_like(ref)
            y_table(z, place, ytab)
            z_tables(z, place, ztab)
        def send_up(distance):
            @pl.when(gz + distance < n_gz)
            def _():
                pl.semaphore_wait(ready.at[n_gz - distance - 1], 1)
                copy_z(n_gz - distance).start()

        send_up(1)
        wait_z(1)
        for distance in range(2, n_gz):
            send_up(distance)

        def arrive(r, g):
            def blocks_in(ref):
                pltpu.make_async_copy(ref, ref, recv_c.at[r * z.groups + g]).wait()

            with jax.named_scope("x_wait"):
                first = lambda: blocks_in(cols.at[r, pl.ds(1, z.per - 1)])
                if z.groups == 1:
                    first()
                else:
                    pl.when(g == 0)(first)

                    @pl.when(g > 0)
                    def _():
                        blocks_in(cols.at[r, pl.ds(g * z.per, z.per)])

            unpack(z, [cols[r, g * z.per + d] for d in range(z.per)], prm)

        lower = gz < n_gz // 2

        def second():
            for r in range(2, n_gz - 1):
                wait_z(r)

            @pl.when(lower)
            def _():
                wait_z(n_gz - 1)

        def third():
            @pl.when(jnp.logical_not(lower))
            def _():
                wait_z(n_gz - 1)

        def chunk(c, carry):
            r, g = c // z.groups, c % z.groups
            arrive(r, g)
            pl.when(c == z.groups)(third)
            with jax.named_scope("chunk"):
                chunk_work(z, place, r, prm, s)
            pl.when(c == z.groups - 1)(second)
            with jax.named_scope("dens"):
                density_work(z, place, r, s)
            return carry

        lax.fori_loop(0, n_gz * z.groups - 1, chunk, 0)

        def copy_d(which):
            return pltpu.make_async_remote_copy(
                src_ref=dacc.at[:, pl.ds(which * (CY + HALO), HALO), :],
                dst_ref=edges.at[which],
                send_sem=send_d,
                recv_sem=recv_d.at[0],
                device_id=along_y(2 * which - 1),
                device_id_type=mesh_type,
            )

        half = z.rows // 2

        def copy_e(dy, part):
            rows = pl.ds(part * half, half)
            return pltpu.make_async_remote_copy(
                src_ref=give.at[dy - 1, rows],
                dst_ref=got.at[dy - 1, rows],
                send_sem=send_e,
                recv_sem=recv_e.at[dy - 1],
                device_id=along_y(dy),
                device_id_type=mesh_type,
            )

        loads[-1].wait()

        def x_transform(g):
            v = acc[2 * z.wide * g : 2 * z.wide * (g + 1)]
            hi, lo = split(v)
            for kk in range(z.kys):
                parts = [
                    w[m * z.wide + kk * z.nx : m * z.wide + (kk + 1) * z.nx]
                    for w in (hi, lo, hi)
                    for m in range(2)
                ]
                q = jnp.dot(xt[...], jnp.concatenate(parts, axis=0), preferred_element_type=f32)
                out = q[: z.nx] + swapped(z, q[z.nx :])
                start = g * z.wide + kk * z.nx
                rows = slice(start, start + z.nx)
                own[rows] = out[:, : 2 * z.nkz]
                for dy in range(1, n_gy):
                    give[dy - 1, rows] = out[:, 2 * z.nkz * dy : 2 * z.nkz * (dy + 1)]

        arrive(n_gz - 1, z.groups - 1)
        with jax.named_scope("last"):
            chunk_work(z, place, n_gz - 1, prm, s, x_transform)
        for which in range(2):
            copy_d(which).start()
        for part in range(2):
            for g in range(z.blocks // 2):
                x_transform(part * z.blocks // 2 + g)
            for dy in range(1, n_gy):
                copy_e(dy, part).start()

        def done(ref, sem):
            pltpu.make_async_copy(ref, ref, sem).wait()

        with jax.named_scope("drain"):
            done(cols.at[0, pl.ds(0, n_gz - 1)], send_z)
            done(cols.at[:, pl.ds(1, n_gx - 1)], send_c)
        with jax.named_scope("exchange_wait"):
            done(edges, send_d)
            done(edges, recv_d.at[0])
            done(give, send_e)
            for dy in range(1, n_gy):
                done(got.at[dy - 1], recv_e.at[dy - 1])

    pl.run_scoped(
        body,
        pltpu.VMEM((2 * z.nky, 3 * CYW), bf16),
        pltpu.VMEM((n_gz, z.cols, 3 * CZW), bf16),
        *[pltpu.VMEM((2 * z.wide, 3 * DEPTH), bf16)] * TS,
        pltpu.VMEM((z.cols, 3 * DEPTH), bf16),
        pltpu.VMEM((CX * CYW, 3 * DEPTH), bf16),
        pltpu.VMEM((3 * CZW, DEPTH), bf16),
        pltpu.VMEM((3 * CYW, DEPTH), bf16),
        pltpu.VMEM((CX * HALO, 3 * DEPTH), bf16),
    )


def add_edges(dacc, eacc):
    lane = lax.broadcasted_iota(jnp.int32, (CYW, LANES), 1)
    pad = jnp.zeros((CYW, LANES - CX * HALO), f32)
    for which, start in ((0, LANES - HALO), (1, 0)):
        e = jnp.concatenate([eacc[which], pad], axis=1)
        mask = (lane >= start) & (lane < start + HALO)
        for x in range(CX):
            v = pltpu.roll(e, (start - x * HALO) % LANES, 1)
            dacc[x] = dacc[x] + jnp.where(mask, v, 0.0)


def finish(z, own, got, dacc, edges, dens_ref, spec_ref):
    total = own[...]
    for dy in range(1, z.n_gy):
        total = total + got[dy - 1]
    spec_ref[0] = total[:, : z.nkz]
    spec_ref[1] = total[:, z.nkz :]
    dens_ref[...] = dacc[:, HALO : HALO + CY]
    dens_ref[:, CY - HALO :] = dens_ref[:, CY - HALO :] + edges[0]
    dens_ref[:, :HALO] = dens_ref[:, :HALO] + edges[1]


def x_table(z):
    idx = np.arange(z.nx)
    angle = (idx[:, None] * idx[None, :] % z.nx) * (2.0 * math.pi / z.nx)
    c, s = np.cos(angle), np.sin(angle)
    full = np.block([[c, s], [s, -c]]) / math.sqrt(z.nx * z.ny * z.nz)
    full = full.astype(np.float32)
    hi = full.astype(ml_dtypes.bfloat16)
    lo = (full - hi.astype(np.float32)).astype(ml_dtypes.bfloat16)
    return np.concatenate([hi, hi, lo], axis=1)


def shards(
    pair_blocks, basis_map, pair_cells, pair_offsets, exponent_index, radius_index, exponents
):
    n_gx, n_gy, n_gz = (lax.axis_size(a) for a in ("gx", "gy", "gz"))
    pair_dev = pair_blocks.shape[1]
    z = Sizes(n_gx, n_gy, n_gz, pair_dev)
    assert FOLD * pair_dev == LANES and n_gx % z.per == 0 and n_gz >= 3 and n_gy >= 2 and z.blocks % 2 == 0
    assert n_gx >= n_gz
    in_vmem = pl.BlockSpec(memory_space=pltpu.VMEM)
    in_hbm = pl.BlockSpec(memory_space=pltpu.HBM)
    basis = basis_map.T
    blocks = pair_blocks.T
    xt = jnp.asarray(x_table(z))
    ei, ri = exponent_index.reshape(1, -1), radius_index.reshape(1, -1)
    dma = pltpu.SemaphoreType.DMA
    own, got, dacc, edges = pl.pallas_call(
        functools.partial(kernel, z),
        out_shape=[
            jax.ShapeDtypeStruct((z.rows, 2 * z.nkz), f32),
            jax.ShapeDtypeStruct((n_gy - 1, z.rows, 2 * z.nkz), f32),
            jax.ShapeDtypeStruct((CX, CYW, CZ), f32),
            jax.ShapeDtypeStruct((2, CX, HALO, CZ), f32),
        ],
        in_specs=[in_hbm] * 8,
        out_specs=[in_vmem] * 4,
        scratch_shapes=[
            pltpu.VMEM(basis.shape, f32),
            pltpu.VMEM(blocks.shape, f32),
            pltpu.VMEM(pair_cells.shape, jnp.int32),
            pltpu.VMEM(pair_offsets.shape, f32),
            pltpu.VMEM(ei.shape, jnp.int32),
            pltpu.VMEM(ri.shape, jnp.int32),
            pltpu.SMEM(exponents.shape, f32),
            pltpu.VMEM(xt.shape, bf16),
            pltpu.VMEM((8, LANES), f32),
            pltpu.VMEM((COEFS + 8, LANES), f32),
            pltpu.VMEM((n_gz, n_gx, BLOCK_ROWS, LANES), f32),
            pltpu.VMEM((n_gy - 1, z.rows, 2 * z.nkz), f32),
            pltpu.VMEM((SIDE * SIDE, z.blocks, 2 * z.kys, LANES), f32),
            pltpu.VMEM((SIDE * SIDE, CX, LANES), f32),
            pltpu.VMEM((SIDE, CYW, LANES), f32),
            pltpu.VMEM((2, SIDE, HALO, LANES), f32),
            pltpu.VMEM((2 * z.rows, z.cols), f32),
            pltpu.VMEM((2, CYW, CX * HALO), f32),
            pltpu.SemaphoreType.REGULAR((n_gz - 1,)),
            dma((8,)),
            dma((n_gz - 1,)),
            dma((n_gz * z.groups,)),
            dma((n_gy - 1,)),
            dma((1,)),
        ],
        compiler_params=pltpu.CompilerParams(
            collective_id=0, has_side_effects=True, vmem_limit_bytes=VMEM_LIMIT
        ),
    )(
        *(
            pltpu.with_memory_space_constraint(a, pltpu.HBM)
            for a in (basis, blocks, pair_cells, pair_offsets, ei, ri, exponents, xt)
        )
    )
    dens, spec = pl.pallas_call(
        functools.partial(finish, z),
        out_shape=[
            jax.ShapeDtypeStruct((CX, CY, CZ), f32),
            jax.ShapeDtypeStruct((2, z.rows, z.nkz), f32),
        ],
        in_specs=[in_vmem] * 4,
        out_specs=[in_vmem] * 2,
        compiler_params=pltpu.CompilerParams(vmem_limit_bytes=VMEM_LIMIT),
    )(own, got, dacc, edges)
    return dens, spec.reshape(2, z.nky, z.nx, z.nkz).transpose(0, 3, 1, 2)


def solution(mesh):
    placed = (
        P(None, ("gx", "gy", "gz")),
        P(),
        P(None, ("gx", "gy", "gz")),
        P(None, ("gx", "gy", "gz")),
        P(("gx", "gy", "gz")),
        P(("gx", "gy", "gz")),
        P(),
    )
    return jax.shard_map(
        shards,
        mesh=mesh,
        in_specs=placed,
        out_specs=(P("gx", "gy", "gz"), P(None, ("gy", "gz"), "gx", None)),
        check_vma=False,
    )
```

```python
import functools
import math

import jax
import jax.numpy as jnp
import ml_dtypes
import numpy as np
from jax import lax
from jax.experimental import pallas as pl
from jax.experimental.pallas import tpu as pltpu
from jax.sharding import PartitionSpec as P

DEG = 3
HALO = 8
CX = 8
CY = 32
CZ = 128
SIDE = DEG + 1
LANES = 128
VMEM_LIMIT = 40 << 20
COEFS = SIDE**3
FOLD = 4
TOP = COEFS // FOLD
BLOCK_ROWS = TOP + 8
CYW = CY + 2 * HALO
CZW = CZ + 2 * HALO
TS = 4
DEPTH = SIDE * LANES

f32 = jnp.float32
bf16 = jnp.bfloat16


def iota_f(shape, dim):
    return lax.broadcasted_iota(jnp.int32, shape, dim).astype(f32)


def cos_sin(turns):
    r = turns - jnp.floor(turns + 0.5)
    t = r * math.pi
    t2 = t * t
    s = t * _poly(t2, [(-1) ** n / math.factorial(2 * n + 1) for n in range(7)])
    c = _poly(t2, [(-1) ** n / math.factorial(2 * n) for n in range(8)])
    return 1.0 - 2.0 * s * s, 2.0 * s * c


def _poly(x, coefs):
    out = jnp.full_like(x, coefs[-1])
    for a in reversed(coefs[:-1]):
        out = out * x + a
    return out


def wrapped(cells, centre, total):
    d = cells - centre
    d = jnp.where(d < -HALO, d + total, d)
    return jnp.where(d > total - 1 - HALO, d - total, d)


def factors(offset, within, fall, radius):
    u = offset - within
    env = jnp.where(jnp.abs(offset) <= radius, jnp.exp2(fall * (u * u)), 0.0)
    s = u * (1.0 / HALO)
    out = [env]
    for _ in range(DEG):
        out.append(out[-1] * s)
    return out


def split(v):
    hi = v.astype(bf16)
    return hi, (v - hi.astype(f32)).astype(bf16)


def nt(a, b):
    return lax.dot_general(a, b, (((1,), (1,)), ((), ())), preferred_element_type=f32)


class Sizes:
    def __init__(self, n_gx, n_gy, n_gz, pair_dev):
        self.n_gx, self.n_gy, self.n_gz = n_gx, n_gy, n_gz
        self.nx, self.ny, self.nz = CX * n_gx, CY * n_gy, CZ * n_gz
        self.nky, self.nkz = self.ny // n_gx, self.nz // (n_gy * n_gz)
        self.pair_dev = pair_dev
        self.per = LANES // pair_dev
        self.groups = n_gx // self.per
        self.wide = max(self.nx, LANES)
        self.kys = self.wide // self.nx
        self.blocks = self.nky // self.kys
        self.cols = 2 * self.nkz * n_gy
        self.rows = self.nky * self.nx


def source_z(z, gz, r):
    step = jnp.where(gz < z.n_gz // 2, r, z.n_gz - r)
    return lax.rem(gz + step, z.n_gz)


def kz_of(z, gy, gz):
    starts = []
    for dy in range(z.n_gy):
        block = lax.rem(gy + dy, z.n_gy) * z.n_gz + gz
        starts.append(iota_f((z.nkz, 1), 0) + (block * z.nkz).astype(f32))
    return jnp.concatenate(starts, axis=0)


def paired(z, a, b):
    n = z.nkz
    out = []
    for dy in range(z.n_gy):
        out += [a[dy * n : (dy + 1) * n], b[dy * n : (dy + 1) * n]]
    return jnp.concatenate(out, axis=0)


def z_tables(z, place, ztab):
    gx, gy, gz = place
    kz = kz_of(z, gy, gz)
    col = lax.broadcasted_iota(jnp.int32, (1, CZW), 1)
    cell = jnp.where(col < CZ + HALO, col, col - CZW).astype(f32)
    c0, s0 = cos_sin(kz * cell * (1.0 / z.nz))
    for r in range(z.n_gz):
        source = source_z(z, gz, r).astype(f32)
        ca, sa = cos_sin(kz * source * (1.0 / z.n_gz))
        c = c0 * ca - s0 * sa
        s = s0 * ca + c0 * sa
        hi, lo = split(paired(z, c, -s))
        ztab[r] = jnp.concatenate([hi, hi, lo], axis=1)


def y_table(z, place, ytab):
    gx, gy, gz = place
    row = lax.broadcasted_iota(jnp.int32, (2 * z.nky, 1), 0)
    ky = (row // (2 * z.kys) * z.kys + row % z.kys + gx * z.nky).astype(f32)
    y = iota_f((1, CYW), 1) + ((gy * CY).astype(f32) - HALO)
    c, s = cos_sin(ky * y * (1.0 / z.ny))
    hi, lo = split(jnp.where(row % (2 * z.kys) < z.kys, c, -s))
    ytab[...] = jnp.concatenate([hi, hi, lo], axis=1)


def put3(ref, rows, k, hi, lo, order):
    for n, which in enumerate(order):
        ref[rows, n * DEPTH + k * LANES : n * DEPTH + (k + 1) * LANES] = lo if which else hi


def stack3(ref, k, v):
    hi, lo = split(v)
    n = v.shape[0]
    lanes = slice(k * LANES, (k + 1) * LANES)
    ref[:n, lanes] = hi
    ref[n : 2 * n, lanes] = lo
    ref[2 * n :, lanes] = hi


def chunk_work(z, place, r, prm, s, after=None):
    gx, gy, gz = place
    row = lambda a: prm[a : a + 1, :]
    cx, cy, cz, ox, oy, oz, rate, radius = [row(COEFS + n) for n in range(8)]
    fall = rate * (-1.0 / math.log(2.0))
    nx = z.nx

    fy = factors(iota_f((CYW, LANES), 0) + ((gy * CY).astype(f32) - HALO) - cy, oy, fall, radius)
    for j in range(SIDE):
        s.fy[j] = fy[j]
        stack3(s.yw, j, fy[j])
    part = jnp.dot(s.ytab[...], s.yw[...], preferred_element_type=f32)
    for k in range(SIDE):
        for i in range(SIDE):
            v = None
            for j in range(SIDE):
                w = row((i * SIDE + j) * SIDE + k) * part[:, j * LANES : (j + 1) * LANES]
                v = w if v is None else v + w
            for g in range(z.blocks):
                s.h[k * SIDE + i, g] = v[2 * z.kys * g : 2 * z.kys * (g + 1)]

    fx = factors(wrapped(iota_f((nx, LANES), 0), cx, float(z.nx)), ox, fall, radius)
    fxl = factors(
        wrapped(iota_f((CX, LANES), 0) + (gx * CX).astype(f32), cx, float(z.nx)), ox, fall, radius
    )
    for k in range(SIDE):
        for j in range(SIDE):
            v = None
            for i in range(SIDE):
                w = row((i * SIDE + j) * SIDE + k) * fxl[i]
                v = w if v is None else v + w
            s.hd[k * SIDE + j] = v

    cell = lax.broadcasted_iota(jnp.int32, (CZW, LANES), 0)
    cell = jnp.where(cell < CZ + HALO, cell, cell - CZW).astype(f32)
    source = source_z(z, gz, r) * CZ
    fz = factors(cell - (cz - source.astype(f32)), oz, fall, radius)
    for k in range(SIDE):
        s.fe[0, k] = fz[k][CZ + HALO :]
        s.fe[1, k] = fz[k][CZ : CZ + HALO]
        stack3(s.zw, k, fz[k])
    for k in range(0, SIDE, 2):
        two = s.zw[:, k * LANES : (k + 2) * LANES]
        v = jnp.dot(s.ztab[r], two, preferred_element_type=f32)
        for n in range(2):
            hi, lo = split(v[:, n * LANES : (n + 1) * LANES])
            put3(s.z, slice(0, z.cols), k + n, hi, lo, (0, 0, 1))

    def build(g):
        for m in range(2):
            for kk in range(z.kys):
                o = m * z.wide + kk * nx
                for k in range(SIDE):
                    v = None
                    for i in range(SIDE):
                        q = m * z.kys + kk
                        w = s.h[k * SIDE + i, g, q : q + 1, :] * fx[i]
                        v = w if v is None else v + w
                    hi, lo = split(v)
                    put3(s.t[g % TS], slice(o, o + nx), k, hi, lo, (0, 1, 0))

    def product(g):
        rows = slice(2 * z.wide * g, 2 * z.wide * (g + 1))
        s.acc[rows] = s.acc[rows] + nt(s.t[g % TS][...], s.z[...])

    if after is not None:
        density_work(z, place, r, s)
        add_edges(s.dacc, s.eacc)
    build(0)
    for g in range(1, z.blocks):
        build(g)
        product(g - 1)
    product(z.blocks - 1)


def density_work(z, place, r, s):
    near = jnp.where(place[2] < z.n_gz // 2, 0, 1)

    def cells():
        for x in range(CX):
            for k in range(SIDE):
                v = None
                for j in range(SIDE):
                    w = s.hd[k * SIDE + j, x : x + 1, :] * s.fy[j]
                    v = w if v is None else v + w
                hi, lo = split(v)
                put3(s.d, slice(x * CYW, (x + 1) * CYW), k, hi, lo, (0, 1, 0))
        hi, lo = s.zw[:CZ], s.zw[CZW : CZW + CZ]
        more = nt(s.d[...], jnp.concatenate([hi, hi, lo], axis=1))
        s.dacc[...] = s.dacc[...] + more.reshape(CX, CYW, CZ)

    def edge(which):
        for x in range(0, CX, 2):
            for j in range(SIDE):
                both = []
                for xx in (x, x + 1):
                    v = None
                    for k in range(SIDE):
                        w = s.hd[k * SIDE + j, xx : xx + 1, :] * s.fe[which, k]
                        v = w if v is None else v + w
                    both.append(v)
                hi, lo = split(jnp.concatenate(both, axis=0))
                put3(s.te, slice(x * HALO, (x + 2) * HALO), j, hi, lo, (0, 0, 1))
        hi, lo = s.yw[:CYW], s.yw[CYW : 2 * CYW]
        more = nt(jnp.concatenate([hi, lo, hi], axis=1), s.te[...])
        s.eacc[which] = s.eacc[which] + more

    if isinstance(r, int):
        edge(1 - near)
        return
    pl.when(r == 0)(cells)
    pl.when(r == 1)(lambda: edge(near))
    if z.groups > 1:
        pl.when(r == z.n_gz - 1)(lambda: edge(1 - near))


class Scratch:
    pass


def params_of(z, cells, offs, e_index, r_index, exponents, pm):
    n = z.pair_dev
    pm[...] = jnp.zeros_like(pm)
    radius = (HALO - r_index[...]).astype(f32)
    chosen = None
    for e in range(exponents.shape[0]):
        w = jnp.where(e_index[...] == e, exponents[e], 0.0)
        chosen = w if chosen is None else chosen + w
    pm[0:3, :n] = cells[...].astype(f32)
    pm[3:6, :n] = offs[...]
    pm[6:7, :n] = chosen / (radius * radius)
    pm[7:8, :n] = radius


def coefficients(z, basis, blocks):
    bh, bl = split(basis[...])
    ph, pb = split(blocks[...])
    both = nt(jnp.concatenate([bh, bl], axis=0), ph)
    v = both[:COEFS] + (both[COEFS:] + nt(bh, pb))
    return jnp.concatenate([v[g * TOP : (g + 1) * TOP] for g in range(FOLD)], axis=1)


def unpack(z, blocks, prm):
    owner = lax.broadcasted_iota(jnp.int32, (TOP, LANES), 1) // z.pair_dev
    for g in range(FOLD):
        v = None
        for d, block in enumerate(blocks):
            shift = (d - g) % FOLD * z.pair_dev
            w = block[:TOP]
            w = pltpu.roll(w, shift, 1) if shift else w
            v = w if v is None else jnp.where(owner == d, w, v)
        prm[g * TOP : (g + 1) * TOP] = v
    v = None
    for d, block in enumerate(blocks):
        w = block[TOP:]
        w = pltpu.roll(w, d * z.pair_dev, 1) if d else w
        v = w if v is None else jnp.where(owner[:8] == d, w, v)
    prm[COEFS : COEFS + 8] = v


def swapped(z, b):
    lane = lax.broadcasted_iota(jnp.int32, (b.shape[0], LANES), 1)
    first = lane % (2 * z.nkz) < z.nkz
    out = []
    for c in range(z.cols // LANES):
        w = b[:, c * LANES : (c + 1) * LANES]
        down = pltpu.roll(w, LANES - z.nkz, 1)
        up = down if 2 * z.nkz == LANES else pltpu.roll(w, z.nkz, 1)
        out.append(jnp.where(first, down, -up))
    return jnp.concatenate(out, axis=1)


def kernel(
    z, basis_hbm, blocks_hbm, cells_hbm, offs_hbm, ei_hbm, ri_hbm, ex_hbm, xt_hbm,
    own, got, dacc, edges,
    basis, blocks, cells, offs, e_index, r_index, exponents, xt, pm, prm, cols, give,
    h, hd, fy, fe, acc, eacc,
    ready, in_sem, recv_z, recv_c, recv_e, recv_d,
):
    n_gx, n_gy, n_gz = z.n_gx, z.n_gy, z.n_gz
    gx, gy, gz = (lax.axis_index(a) for a in ("gx", "gy", "gz"))
    place = gx, gy, gz
    mesh_type = pl.DeviceIdType.MESH

    def along_z(r):
        return gx, gy, lax.rem(gz + n_gz - r, n_gz)

    def along_x(dx):
        return lax.rem(gx + n_gx - dx, n_gx), gy, gz

    def along_y(dy):
        return gx, lax.rem(gy + n_gy + dy, n_gy), gz

    barrier = pltpu.get_barrier_semaphore()
    for r in range(1, n_gz):

        @pl.when(r > gz)
        def _(r=r):
            pl.semaphore_signal(barrier, inc=1, device_id=along_z(r), device_id_type=mesh_type)

    def greet(dx, carry):
        pl.semaphore_signal(barrier, inc=1, device_id=along_x(dx), device_id_type=mesh_type)
        return carry

    lax.fori_loop(1, n_gx, greet, 0)
    for dy in range(1, n_gy):
        pl.semaphore_signal(barrier, inc=1, device_id=along_y(dy), device_id_type=mesh_type)

    pairs = [
        (blocks_hbm, blocks), (basis_hbm, basis), (cells_hbm, cells), (offs_hbm, offs),
        (ei_hbm, e_index), (ri_hbm, r_index), (ex_hbm, exponents), (xt_hbm, xt),
    ]
    loads = [
        pltpu.make_async_copy(a, b, in_sem.at[n]) for n, (a, b) in enumerate(pairs)
    ]
    for c in loads:
        c.start()
    with jax.named_scope("load_wait"):
        for c in loads[:-1]:
            c.wait()
    with jax.named_scope("coefs"):
        params_of(z, cells, offs, e_index, r_index, exponents, pm)
        cols[0, 0, :TOP] = coefficients(z, basis, blocks)
        cols[0, 0, TOP:] = pm[...]

    def body(ytab, ztab, t0, t1, t2, t3, zs, d, zw, yw, te):
        s = Scratch()
        s.ytab, s.ztab, s.t, s.z = ytab, ztab, (t0, t1, t2, t3), zs
        s.d, s.zw, s.yw, s.te = d, zw, yw, te
        s.h, s.hd, s.fy, s.fe = h, hd, fy, fe
        s.acc, s.dacc, s.eacc = acc, dacc, eacc
        with jax.named_scope("barrier_wait"):
            pl.semaphore_wait(barrier, n_gx + n_gy - 2 + gz)

        send_z, send_c, send_e, send_d = (in_sem.at[n] for n in range(4))

        def copy_z(q):
            target = along_z(q)
            slot = jnp.where(target[2] < n_gz // 2, q, n_gz - q)
            return pltpu.make_async_remote_copy(
                src_ref=cols.at[0, 0],
                dst_ref=cols.at[slot, 0],
                send_sem=send_z,
                recv_sem=recv_z.at[slot - 1],
                device_id=target,
                device_id_type=mesh_type,
            )

        def wait_z(r):
            with jax.named_scope(f"z_wait{r}"):
                pltpu.make_async_remote_copy(
                    src_ref=cols.at[0, 0],
                    dst_ref=cols.at[r, 0],
                    send_sem=send_z,
                    recv_sem=recv_z.at[r - 1],
                    device_id=along_z(r),
                    device_id_type=mesh_type,
                ).wait_recv()
            forward(r)

        def copy_c(r, dx):
            return pltpu.make_async_remote_copy(
                src_ref=cols.at[r, 0],
                dst_ref=cols.at[r, dx],
                send_sem=send_c,
                recv_sem=recv_c.at[r * z.groups + dx // z.per],
                device_id=along_x(dx),
                device_id_type=mesh_type,
            )

        def forward(r):
            def one(dx, carry):
                copy_c(r, dx).start()
                return carry

            lax.fori_loop(1, n_gx, one, 0)

        for r in range(1, n_gz):

            @pl.when(r <= gz)
            def _(r=r):
                pl.semaphore_signal(
                    ready.at[n_gz - r - 1], inc=1, device_id=along_z(r), device_id_type=mesh_type
                )
                copy_z(r).start()

        forward(0)
        with jax.named_scope("tables"):
            for ref in (acc, dacc, eacc):
                ref[...] = jnp.zeros_like(ref)
            y_table(z, place, ytab)
            z_tables(z, place, ztab)
        def send_up(distance):
            @pl.when(gz + distance < n_gz)
            def _():
                pl.semaphore_wait(ready.at[n_gz - distance - 1], 1)
                copy_z(n_gz - distance).start()

        send_up(1)
        wait_z(1)
        for distance in range(2, n_gz):
            send_up(distance)

        def arrive(r, g):
            def blocks_in(ref):
                pltpu.make_async_copy(ref, ref, recv_c.at[r * z.groups + g]).wait()

            with jax.named_scope("x_wait"):
                first = lambda: blocks_in(cols.at[r, pl.ds(1, z.per - 1)])
                if z.groups == 1:
                    first()
                else:
                    pl.when(g == 0)(first)

                    @pl.when(g > 0)
                    def _():
                        blocks_in(cols.at[r, pl.ds(g * z.per, z.per)])

            unpack(z, [cols[r, g * z.per + d] for d in range(z.per)], prm)

        lower = gz < n_gz // 2

        def second():
            for r in range(2, n_gz - 1):
                wait_z(r)

            @pl.when(lower)
            def _():
                wait_z(n_gz - 1)

        def third():
            @pl.when(jnp.logical_not(lower))
            def _():
                wait_z(n_gz - 1)

        def chunk(c, carry):
            r, g = c // z.groups, c % z.groups
            arrive(r, g)
            pl.when(c == z.groups)(third)
            with jax.named_scope("chunk"):
                chunk_work(z, place, r, prm, s)
            pl.when(c == z.groups - 1)(second)
            with jax.named_scope("dens"):
                density_work(z, place, r, s)
            return carry

        lax.fori_loop(0, n_gz * z.groups - 1, chunk, 0)

        def copy_d(which):
            return pltpu.make_async_remote_copy(
                src_ref=dacc.at[:, pl.ds(which * (CY + HALO), HALO), :],
                dst_ref=edges.at[which],
                send_sem=send_d,
                recv_sem=recv_d.at[0],
                device_id=along_y(2 * which - 1),
                device_id_type=mesh_type,
            )

        half = z.rows // 2

        def copy_e(dy, part):
            rows = pl.ds(part * half, half)
            return pltpu.make_async_remote_copy(
                src_ref=give.at[dy - 1, rows],
                dst_ref=got.at[dy - 1, rows],
                send_sem=send_e,
                recv_sem=recv_e.at[dy - 1],
                device_id=along_y(dy),
                device_id_type=mesh_type,
            )

        loads[-1].wait()

        def x_transform(g):
            v = acc[2 * z.wide * g : 2 * z.wide * (g + 1)]
            hi, lo = split(v)
            for kk in range(z.kys):
                parts = [
                    w[m * z.wide + kk * z.nx : m * z.wide + (kk + 1) * z.nx]
                    for w in (hi, lo, hi)
                    for m in range(2)
                ]
                q = jnp.dot(xt[...], jnp.concatenate(parts, axis=0), preferred_element_type=f32)
                out = q[: z.nx] + swapped(z, q[z.nx :])
                start = g * z.wide + kk * z.nx
                rows = slice(start, start + z.nx)
                own[rows] = out[:, : 2 * z.nkz]
                for dy in range(1, n_gy):
                    give[dy - 1, rows] = out[:, 2 * z.nkz * dy : 2 * z.nkz * (dy + 1)]

        arrive(n_gz - 1, z.groups - 1)
        with jax.named_scope("last"):
            chunk_work(z, place, n_gz - 1, prm, s, x_transform)
        for which in range(2):
            copy_d(which).start()
        for part in range(2):
            for g in range(z.blocks // 2):
                x_transform(part * z.blocks // 2 + g)
            for dy in range(1, n_gy):
                copy_e(dy, part).start()

        def done(ref, sem):
            pltpu.make_async_copy(ref, ref, sem).wait()

        with jax.named_scope("drain"):
            done(cols.at[0, pl.ds(0, n_gz - 1)], send_z)
            done(cols.at[:, pl.ds(1, n_gx - 1)], send_c)
        with jax.named_scope("exchange_wait"):
            done(edges, send_d)
            done(edges, recv_d.at[0])
            done(give, send_e)
            for dy in range(1, n_gy):
                done(got.at[dy - 1], recv_e.at[dy - 1])

    pl.run_scoped(
        body,
        pltpu.VMEM((2 * z.nky, 3 * CYW), bf16),
        pltpu.VMEM((n_gz, z.cols, 3 * CZW), bf16),
        *[pltpu.VMEM((2 * z.wide, 3 * DEPTH), bf16)] * TS,
        pltpu.VMEM((z.cols, 3 * DEPTH), bf16),
        pltpu.VMEM((CX * CYW, 3 * DEPTH), bf16),
        pltpu.VMEM((3 * CZW, DEPTH), bf16),
        pltpu.VMEM((3 * CYW, DEPTH), bf16),
        pltpu.VMEM((CX * HALO, 3 * DEPTH), bf16),
    )


def add_edges(dacc, eacc):
    lane = lax.broadcasted_iota(jnp.int32, (CYW, LANES), 1)
    pad = jnp.zeros((CYW, LANES - CX * HALO), f32)
    for which, start in ((0, LANES - HALO), (1, 0)):
        e = jnp.concatenate([eacc[which], pad], axis=1)
        mask = (lane >= start) & (lane < start + HALO)
        for x in range(CX):
            v = pltpu.roll(e, (start - x * HALO) % LANES, 1)
            dacc[x] = dacc[x] + jnp.where(mask, v, 0.0)


def finish(z, own, got, dacc, edges, dens_ref, spec_ref):
    total = own[...]
    for dy in range(1, z.n_gy):
        total = total + got[dy - 1]
    spec_ref[0] = total[:, : z.nkz]
    spec_ref[1] = total[:, z.nkz :]
    dens_ref[...] = dacc[:, HALO : HALO + CY]
    dens_ref[:, CY - HALO :] = dens_ref[:, CY - HALO :] + edges[0]
    dens_ref[:, :HALO] = dens_ref[:, :HALO] + edges[1]


def x_table(z):
    idx = np.arange(z.nx)
    angle = (idx[:, None] * idx[None, :] % z.nx) * (2.0 * math.pi / z.nx)
    c, s = np.cos(angle), np.sin(angle)
    full = np.block([[c, s], [s, -c]]) / math.sqrt(z.nx * z.ny * z.nz)
    full = full.astype(np.float32)
    hi = full.astype(ml_dtypes.bfloat16)
    lo = (full - hi.astype(np.float32)).astype(ml_dtypes.bfloat16)
    return np.concatenate([hi, hi, lo], axis=1)


def shards(
    pair_blocks, basis_map, pair_cells, pair_offsets, exponent_index, radius_index, exponents
):
    n_gx, n_gy, n_gz = (lax.axis_size(a) for a in ("gx", "gy", "gz"))
    pair_dev = pair_blocks.shape[1]
    z = Sizes(n_gx, n_gy, n_gz, pair_dev)
    assert FOLD * pair_dev == LANES and n_gx % z.per == 0 and n_gz >= 3 and n_gy >= 2 and z.blocks % 2 == 0
    assert n_gx >= n_gz
    in_vmem = pl.BlockSpec(memory_space=pltpu.VMEM)
    in_hbm = pl.BlockSpec(memory_space=pltpu.HBM)
    basis = basis_map.T
    blocks = pair_blocks.T
    xt = jnp.asarray(x_table(z))
    ei, ri = exponent_index.reshape(1, -1), radius_index.reshape(1, -1)
    dma = pltpu.SemaphoreType.DMA
    own, got, dacc, edges = pl.pallas_call(
        functools.partial(kernel, z),
        out_shape=[
            jax.ShapeDtypeStruct((z.rows, 2 * z.nkz), f32),
            jax.ShapeDtypeStruct((n_gy - 1, z.rows, 2 * z.nkz), f32),
            jax.ShapeDtypeStruct((CX, CYW, CZ), f32),
            jax.ShapeDtypeStruct((2, CX, HALO, CZ), f32),
        ],
        in_specs=[in_hbm] * 8,
        out_specs=[in_vmem] * 4,
        scratch_shapes=[
            pltpu.VMEM(basis.shape, f32),
            pltpu.VMEM(blocks.shape, f32),
            pltpu.VMEM(pair_cells.shape, jnp.int32),
            pltpu.VMEM(pair_offsets.shape, f32),
            pltpu.VMEM(ei.shape, jnp.int32),
            pltpu.VMEM(ri.shape, jnp.int32),
            pltpu.SMEM(exponents.shape, f32),
            pltpu.VMEM(xt.shape, bf16),
            pltpu.VMEM((8, LANES), f32),
            pltpu.VMEM((COEFS + 8, LANES), f32),
            pltpu.VMEM((n_gz, n_gx, BLOCK_ROWS, LANES), f32),
            pltpu.VMEM((n_gy - 1, z.rows, 2 * z.nkz), f32),
            pltpu.VMEM((SIDE * SIDE, z.blocks, 2 * z.kys, LANES), f32),
            pltpu.VMEM((SIDE * SIDE, CX, LANES), f32),
            pltpu.VMEM((SIDE, CYW, LANES), f32),
            pltpu.VMEM((2, SIDE, HALO, LANES), f32),
            pltpu.VMEM((2 * z.rows, z.cols), f32),
            pltpu.VMEM((2, CYW, CX * HALO), f32),
            pltpu.SemaphoreType.REGULAR((n_gz - 1,)),
            dma((8,)),
            dma((n_gz - 1,)),
            dma((n_gz * z.groups,)),
            dma((n_gy - 1,)),
            dma((1,)),
        ],
        compiler_params=pltpu.CompilerParams(
            collective_id=0, has_side_effects=True, vmem_limit_bytes=VMEM_LIMIT
        ),
    )(
        *(
            pltpu.with_memory_space_constraint(a, pltpu.HBM)
            for a in (basis, blocks, pair_cells, pair_offsets, ei, ri, exponents, xt)
        )
    )
    dens, spec = pl.pallas_call(
        functools.partial(finish, z),
        out_shape=[
            jax.ShapeDtypeStruct((CX, CY, CZ), f32),
            jax.ShapeDtypeStruct((2, z.rows, z.nkz), f32),
        ],
        in_specs=[in_vmem] * 4,
        out_specs=[in_vmem] * 2,
        compiler_params=pltpu.CompilerParams(vmem_limit_bytes=VMEM_LIMIT),
    )(own, got, dacc, edges)
    return dens, spec.reshape(2, z.nky, z.nx, z.nkz).transpose(0, 3, 1, 2)


def solution(mesh):
    placed = (
        P(None, ("gx", "gy", "gz")),
        P(),
        P(None, ("gx", "gy", "gz")),
        P(None, ("gx", "gy", "gz")),
        P(("gx", "gy", "gz")),
        P(("gx", "gy", "gz")),
        P(),
    )
    return jax.shard_map(
        shards,
        mesh=mesh,
        in_specs=placed,
        out_specs=(P("gx", "gy", "gz"), P(None, ("gy", "gz"), "gx", None)),
        check_vma=False,
    )
```

```python
import functools
import math

import jax
import jax.numpy as jnp
import ml_dtypes
import numpy as np
from jax import lax
from jax.experimental import pallas as pl
from jax.experimental.pallas import tpu as pltpu
from jax.sharding import PartitionSpec as P

DEG = 3
HALO = 8
CX = 8
CY = 32
CZ = 128
SIDE = DEG + 1
LANES = 128
VMEM_LIMIT = 40 << 20
COEFS = SIDE**3
FOLD = 4
TOP = COEFS // FOLD
BLOCK_ROWS = TOP + 8
CYW = CY + 2 * HALO
CZW = CZ + 2 * HALO
TS = 4
DEPTH = SIDE * LANES

f32 = jnp.float32
bf16 = jnp.bfloat16


def iota_f(shape, dim):
    return lax.broadcasted_iota(jnp.int32, shape, dim).astype(f32)


def cos_sin(turns):
    r = turns - jnp.floor(turns + 0.5)
    t = r * math.pi
    t2 = t * t
    s = t * _poly(t2, [(-1) ** n / math.factorial(2 * n + 1) for n in range(7)])
    c = _poly(t2, [(-1) ** n / math.factorial(2 * n) for n in range(8)])
    return 1.0 - 2.0 * s * s, 2.0 * s * c


def _poly(x, coefs):
    out = jnp.full_like(x, coefs[-1])
    for a in reversed(coefs[:-1]):
        out = out * x + a
    return out


def wrapped(cells, centre, total):
    d = cells - centre
    d = jnp.where(d < -HALO, d + total, d)
    return jnp.where(d > total - 1 - HALO, d - total, d)


def factors(offset, within, fall, radius):
    u = offset - within
    env = jnp.where(jnp.abs(offset) <= radius, jnp.exp2(fall * (u * u)), 0.0)
    s = u * (1.0 / HALO)
    out = [env]
    for _ in range(DEG):
        out.append(out[-1] * s)
    return out


def split(v):
    hi = v.astype(bf16)
    return hi, (v - hi.astype(f32)).astype(bf16)


def nt(a, b):
    return lax.dot_general(a, b, (((1,), (1,)), ((), ())), preferred_element_type=f32)


class Sizes:
    def __init__(self, n_gx, n_gy, n_gz, pair_dev):
        self.n_gx, self.n_gy, self.n_gz = n_gx, n_gy, n_gz
        self.nx, self.ny, self.nz = CX * n_gx, CY * n_gy, CZ * n_gz
        self.nky, self.nkz = self.ny // n_gx, self.nz // (n_gy * n_gz)
        self.pair_dev = pair_dev
        self.per = LANES // pair_dev
        self.groups = n_gx // self.per
        self.wide = max(self.nx, LANES)
        self.kys = self.wide // self.nx
        self.blocks = self.nky // self.kys
        self.cols = 2 * self.nkz * n_gy
        self.rows = self.nky * self.nx


def source_z(z, gz, r):
    step = jnp.where(gz < z.n_gz // 2, r, z.n_gz - r)
    return lax.rem(gz + step, z.n_gz)


def kz_of(z, gy, gz):
    starts = []
    for dy in range(z.n_gy):
        block = lax.rem(gy + dy, z.n_gy) * z.n_gz + gz
        starts.append(iota_f((z.nkz, 1), 0) + (block * z.nkz).astype(f32))
    return jnp.concatenate(starts, axis=0)


def paired(z, a, b):
    n = z.nkz
    out = []
    for dy in range(z.n_gy):
        out += [a[dy * n : (dy + 1) * n], b[dy * n : (dy + 1) * n]]
    return jnp.concatenate(out, axis=0)


def z_tables(z, place, ztab):
    gx, gy, gz = place
    kz = kz_of(z, gy, gz)
    col = lax.broadcasted_iota(jnp.int32, (1, CZW), 1)
    cell = jnp.where(col < CZ + HALO, col, col - CZW).astype(f32)
    c0, s0 = cos_sin(kz * cell * (1.0 / z.nz))
    for r in range(z.n_gz):
        source = source_z(z, gz, r).astype(f32)
        ca, sa = cos_sin(kz * source * (1.0 / z.n_gz))
        c = c0 * ca - s0 * sa
        s = s0 * ca + c0 * sa
        hi, lo = split(paired(z, c, -s))
        ztab[r] = jnp.concatenate([hi, hi, lo], axis=1)


def y_table(z, place, ytab):
    gx, gy, gz = place
    row = lax.broadcasted_iota(jnp.int32, (2 * z.nky, 1), 0)
    ky = (row // (2 * z.kys) * z.kys + row % z.kys + gx * z.nky).astype(f32)
    y = iota_f((1, CYW), 1) + ((gy * CY).astype(f32) - HALO)
    c, s = cos_sin(ky * y * (1.0 / z.ny))
    hi, lo = split(jnp.where(row % (2 * z.kys) < z.kys, c, -s))
    ytab[...] = jnp.concatenate([hi, hi, lo], axis=1)


def put3(ref, rows, k, hi, lo, order):
    for n, which in enumerate(order):
        ref[rows, n * DEPTH + k * LANES : n * DEPTH + (k + 1) * LANES] = lo if which else hi


def stack3(ref, k, v):
    hi, lo = split(v)
    n = v.shape[0]
    lanes = slice(k * LANES, (k + 1) * LANES)
    ref[:n, lanes] = hi
    ref[n : 2 * n, lanes] = lo
    ref[2 * n :, lanes] = hi


def chunk_work(z, place, r, prm, s, after=None):
    gx, gy, gz = place
    row = lambda a: prm[a : a + 1, :]
    cx, cy, cz, ox, oy, oz, rate, radius = [row(COEFS + n) for n in range(8)]
    fall = rate * (-1.0 / math.log(2.0))
    nx = z.nx

    fy = factors(iota_f((CYW, LANES), 0) + ((gy * CY).astype(f32) - HALO) - cy, oy, fall, radius)
    for j in range(SIDE):
        s.fy[j] = fy[j]
        stack3(s.yw, j, fy[j])
    part = jnp.dot(s.ytab[...], s.yw[...], preferred_element_type=f32)
    for k in range(SIDE):
        for i in range(SIDE):
            v = None
            for j in range(SIDE):
                w = row((i * SIDE + j) * SIDE + k) * part[:, j * LANES : (j + 1) * LANES]
                v = w if v is None else v + w
            for g in range(z.blocks):
                s.h[k * SIDE + i, g] = v[2 * z.kys * g : 2 * z.kys * (g + 1)]

    fx = factors(wrapped(iota_f((nx, LANES), 0), cx, float(z.nx)), ox, fall, radius)
    fxl = factors(
        wrapped(iota_f((CX, LANES), 0) + (gx * CX).astype(f32), cx, float(z.nx)), ox, fall, radius
    )
    for k in range(SIDE):
        for j in range(SIDE):
            v = None
            for i in range(SIDE):
                w = row((i * SIDE + j) * SIDE + k) * fxl[i]
                v = w if v is None else v + w
            s.hd[k * SIDE + j] = v

    cell = lax.broadcasted_iota(jnp.int32, (CZW, LANES), 0)
    cell = jnp.where(cell < CZ + HALO, cell, cell - CZW).astype(f32)
    source = source_z(z, gz, r) * CZ
    fz = factors(cell - (cz - source.astype(f32)), oz, fall, radius)
    for k in range(SIDE):
        s.fe[0, k] = fz[k][CZ + HALO :]
        s.fe[1, k] = fz[k][CZ : CZ + HALO]
        stack3(s.zw, k, fz[k])
    for k in range(0, SIDE, 2):
        two = s.zw[:, k * LANES : (k + 2) * LANES]
        v = jnp.dot(s.ztab[r], two, preferred_element_type=f32)
        for n in range(2):
            hi, lo = split(v[:, n * LANES : (n + 1) * LANES])
            put3(s.z, slice(0, z.cols), k + n, hi, lo, (0, 0, 1))

    def build(g):
        for m in range(2):
            for kk in range(z.kys):
                o = m * z.wide + kk * nx
                for k in range(SIDE):
                    v = None
                    for i in range(SIDE):
                        q = m * z.kys + kk
                        w = s.h[k * SIDE + i, g, q : q + 1, :] * fx[i]
                        v = w if v is None else v + w
                    hi, lo = split(v)
                    put3(s.t[g % TS], slice(o, o + nx), k, hi, lo, (0, 1, 0))

    def product(g):
        rows = slice(2 * z.wide * g, 2 * z.wide * (g + 1))
        s.acc[rows] = s.acc[rows] + nt(s.t[g % TS][...], s.z[...])

    if after is not None:
        density_work(z, place, r, s)
        add_edges(s.dacc, s.eacc)
    else:
        density_work(z, place, r, s, 1)
    build(0)
    for g in range(1, z.blocks):
        build(g)
        product(g - 1)
    product(z.blocks - 1)


def density_work(z, place, r, s, part=0):
    near = jnp.where(place[2] < z.n_gz // 2, 0, 1)

    def cells():
        for x in range(CX):
            for k in range(SIDE):
                v = None
                for j in range(SIDE):
                    w = s.hd[k * SIDE + j, x : x + 1, :] * s.fy[j]
                    v = w if v is None else v + w
                hi, lo = split(v)
                put3(s.d, slice(x * CYW, (x + 1) * CYW), k, hi, lo, (0, 1, 0))
        hi, lo = s.zw[:CZ], s.zw[CZW : CZW + CZ]
        more = nt(s.d[...], jnp.concatenate([hi, hi, lo], axis=1))
        s.dacc[...] = s.dacc[...] + more.reshape(CX, CYW, CZ)

    def edge(which, on=True):
        for x in range(0, CX, 2):
            for j in range(SIDE):
                both = []
                for xx in (x, x + 1):
                    v = None
                    for k in range(SIDE):
                        w = s.hd[k * SIDE + j, xx : xx + 1, :] * s.fe[which, k]
                        v = w if v is None else v + w
                    both.append(v)
                hi, lo = split(jnp.concatenate(both, axis=0))
                put3(s.te, slice(x * HALO, (x + 2) * HALO), j, hi, lo, (0, 0, 1))
        hi, lo = s.yw[:CYW], s.yw[CYW : 2 * CYW]
        more = nt(jnp.concatenate([hi, lo, hi], axis=1), s.te[...])
        s.eacc[which] = s.eacc[which] + jnp.where(on, more, 0.0)

    if isinstance(r, int):
        edge(1 - near)
        return
    if part == 0:
        pl.when(r == 0)(cells)
        return
    far = r == z.n_gz - 1
    edge(jnp.where(far, 1 - near, near), (r == 1) | far)


class Scratch:
    pass


def params_of(z, cells, offs, e_index, r_index, exponents, pm):
    n = z.pair_dev
    pm[...] = jnp.zeros_like(pm)
    radius = (HALO - r_index[...]).astype(f32)
    chosen = None
    for e in range(exponents.shape[0]):
        w = jnp.where(e_index[...] == e, exponents[e], 0.0)
        chosen = w if chosen is None else chosen + w
    pm[0:3, :n] = cells[...].astype(f32)
    pm[3:6, :n] = offs[...]
    pm[6:7, :n] = chosen / (radius * radius)
    pm[7:8, :n] = radius


def coefficients(z, basis, blocks):
    bh, bl = split(basis[...])
    ph, pb = split(blocks[...])
    both = nt(jnp.concatenate([bh, bl], axis=0), ph)
    v = both[:COEFS] + (both[COEFS:] + nt(bh, pb))
    return jnp.concatenate([v[g * TOP : (g + 1) * TOP] for g in range(FOLD)], axis=1)


def unpack(z, blocks, prm):
    owner = lax.broadcasted_iota(jnp.int32, (TOP, LANES), 1) // z.pair_dev
    for g in range(FOLD):
        v = None
        for d, block in enumerate(blocks):
            shift = (d - g) % FOLD * z.pair_dev
            w = block[:TOP]
            w = pltpu.roll(w, shift, 1) if shift else w
            v = w if v is None else jnp.where(owner == d, w, v)
        prm[g * TOP : (g + 1) * TOP] = v
    v = None
    for d, block in enumerate(blocks):
        w = block[TOP:]
        w = pltpu.roll(w, d * z.pair_dev, 1) if d else w
        v = w if v is None else jnp.where(owner[:8] == d, w, v)
    prm[COEFS : COEFS + 8] = v


def swapped(z, b):
    lane = lax.broadcasted_iota(jnp.int32, (b.shape[0], LANES), 1)
    first = lane % (2 * z.nkz) < z.nkz
    out = []
    for c in range(z.cols // LANES):
        w = b[:, c * LANES : (c + 1) * LANES]
        down = pltpu.roll(w, LANES - z.nkz, 1)
        up = down if 2 * z.nkz == LANES else pltpu.roll(w, z.nkz, 1)
        out.append(jnp.where(first, down, -up))
    return jnp.concatenate(out, axis=1)


def kernel(
    z, basis_hbm, blocks_hbm, cells_hbm, offs_hbm, ei_hbm, ri_hbm, ex_hbm, xt_hbm,
    own, got, dacc, edges,
    basis, blocks, cells, offs, e_index, r_index, exponents, xt, pm, prm, cols, give,
    h, hd, fy, fe, acc, eacc,
    ready, in_sem, recv_z, recv_c, recv_e, recv_d,
):
    n_gx, n_gy, n_gz = z.n_gx, z.n_gy, z.n_gz
    gx, gy, gz = (lax.axis_index(a) for a in ("gx", "gy", "gz"))
    place = gx, gy, gz
    mesh_type = pl.DeviceIdType.MESH

    def along_z(r):
        return gx, gy, lax.rem(gz + n_gz - r, n_gz)

    def along_x(dx):
        return lax.rem(gx + n_gx - dx, n_gx), gy, gz

    def along_y(dy):
        return gx, lax.rem(gy + n_gy + dy, n_gy), gz

    barrier = pltpu.get_barrier_semaphore()
    for r in range(1, n_gz):

        @pl.when(r > gz)
        def _(r=r):
            pl.semaphore_signal(barrier, inc=1, device_id=along_z(r), device_id_type=mesh_type)

    def greet(dx, carry):
        pl.semaphore_signal(barrier, inc=1, device_id=along_x(dx), device_id_type=mesh_type)
        return carry

    lax.fori_loop(1, n_gx, greet, 0)
    for dy in range(1, n_gy):
        pl.semaphore_signal(barrier, inc=1, device_id=along_y(dy), device_id_type=mesh_type)

    pairs = [
        (blocks_hbm, blocks), (basis_hbm, basis), (cells_hbm, cells), (offs_hbm, offs),
        (ei_hbm, e_index), (ri_hbm, r_index), (ex_hbm, exponents), (xt_hbm, xt),
    ]
    loads = [
        pltpu.make_async_copy(a, b, in_sem.at[n]) for n, (a, b) in enumerate(pairs)
    ]
    for c in loads:
        c.start()
    with jax.named_scope("load_wait"):
        for c in loads[:-1]:
            c.wait()
    with jax.named_scope("coefs"):
        params_of(z, cells, offs, e_index, r_index, exponents, pm)
        cols[0, 0, :TOP] = coefficients(z, basis, blocks)
        cols[0, 0, TOP:] = pm[...]

    def body(ytab, ztab, t0, t1, t2, t3, zs, d, zw, yw, te):
        s = Scratch()
        s.ytab, s.ztab, s.t, s.z = ytab, ztab, (t0, t1, t2, t3), zs
        s.d, s.zw, s.yw, s.te = d, zw, yw, te
        s.h, s.hd, s.fy, s.fe = h, hd, fy, fe
        s.acc, s.dacc, s.eacc = acc, dacc, eacc
        with jax.named_scope("barrier_wait"):
            pl.semaphore_wait(barrier, n_gx + n_gy - 2 + gz)

        send_z, send_c, send_e, send_d = (in_sem.at[n] for n in range(4))

        def copy_z(q):
            target = along_z(q)
            slot = jnp.where(target[2] < n_gz // 2, q, n_gz - q)
            return pltpu.make_async_remote_copy(
                src_ref=cols.at[0, 0],
                dst_ref=cols.at[slot, 0],
                send_sem=send_z,
                recv_sem=recv_z.at[slot - 1],
                device_id=target,
                device_id_type=mesh_type,
            )

        def wait_z(r):
            with jax.named_scope(f"z_wait{r}"):
                pltpu.make_async_remote_copy(
                    src_ref=cols.at[0, 0],
                    dst_ref=cols.at[r, 0],
                    send_sem=send_z,
                    recv_sem=recv_z.at[r - 1],
                    device_id=along_z(r),
                    device_id_type=mesh_type,
                ).wait_recv()
            forward(r)

        def copy_c(r, dx):
            return pltpu.make_async_remote_copy(
                src_ref=cols.at[r, 0],
                dst_ref=cols.at[r, dx],
                send_sem=send_c,
                recv_sem=recv_c.at[r * z.groups + dx // z.per],
                device_id=along_x(dx),
                device_id_type=mesh_type,
            )

        def forward(r):
            def one(dx, carry):
                copy_c(r, dx).start()
                return carry

            lax.fori_loop(1, n_gx, one, 0)

        for r in range(1, n_gz):

            @pl.when(r <= gz)
            def _(r=r):
                pl.semaphore_signal(
                    ready.at[n_gz - r - 1], inc=1, device_id=along_z(r), device_id_type=mesh_type
                )
                copy_z(r).start()

        forward(0)
        with jax.named_scope("tables"):
            for ref in (acc, dacc, eacc):
                ref[...] = jnp.zeros_like(ref)
            y_table(z, place, ytab)
            z_tables(z, place, ztab)
        def send_up(distance):
            @pl.when(gz + distance < n_gz)
            def _():
                pl.semaphore_wait(ready.at[n_gz - distance - 1], 1)
                copy_z(n_gz - distance).start()

        send_up(1)
        wait_z(1)
        for distance in range(2, n_gz):
            send_up(distance)

        def arrive(r, g):
            def blocks_in(ref):
                pltpu.make_async_copy(ref, ref, recv_c.at[r * z.groups + g]).wait()

            with jax.named_scope("x_wait"):
                first = lambda: blocks_in(cols.at[r, pl.ds(1, z.per - 1)])
                if z.groups == 1:
                    first()
                else:
                    pl.when(g == 0)(first)

                    @pl.when(g > 0)
                    def _():
                        blocks_in(cols.at[r, pl.ds(g * z.per, z.per)])

            unpack(z, [cols[r, g * z.per + d] for d in range(z.per)], prm)

        lower = gz < n_gz // 2

        def second():
            for r in range(2, n_gz - 1):
                wait_z(r)

            @pl.when(lower)
            def _():
                wait_z(n_gz - 1)

        def third():
            @pl.when(jnp.logical_not(lower))
            def _():
                wait_z(n_gz - 1)

        def chunk(c, carry):
            r, g = c // z.groups, c % z.groups
            arrive(r, g)
            pl.when(c == z.groups)(third)
            with jax.named_scope("chunk"):
                chunk_work(z, place, r, prm, s)
            pl.when(c == z.groups - 1)(second)
            with jax.named_scope("dens"):
                density_work(z, place, r, s)
            return carry

        lax.fori_loop(0, n_gz * z.groups - 1, chunk, 0)

        def copy_d(which):
            return pltpu.make_async_remote_copy(
                src_ref=dacc.at[:, pl.ds(which * (CY + HALO), HALO), :],
                dst_ref=edges.at[which],
                send_sem=send_d,
                recv_sem=recv_d.at[0],
                device_id=along_y(2 * which - 1),
                device_id_type=mesh_type,
            )

        half = z.rows // 2

        def copy_e(dy, part):
            rows = pl.ds(part * half, half)
            return pltpu.make_async_remote_copy(
                src_ref=give.at[dy - 1, rows],
                dst_ref=got.at[dy - 1, rows],
                send_sem=send_e,
                recv_sem=recv_e.at[dy - 1],
                device_id=along_y(dy),
                device_id_type=mesh_type,
            )

        loads[-1].wait()

        def x_transform(g):
            v = acc[2 * z.wide * g : 2 * z.wide * (g + 1)]
            hi, lo = split(v)
            for kk in range(z.kys):
                parts = [
                    w[m * z.wide + kk * z.nx : m * z.wide + (kk + 1) * z.nx]
                    for w in (hi, lo, hi)
                    for m in range(2)
                ]
                q = jnp.dot(xt[...], jnp.concatenate(parts, axis=0), preferred_element_type=f32)
                out = q[: z.nx] + swapped(z, q[z.nx :])
                start = g * z.wide + kk * z.nx
                rows = slice(start, start + z.nx)
                own[rows] = out[:, : 2 * z.nkz]
                for dy in range(1, n_gy):
                    give[dy - 1, rows] = out[:, 2 * z.nkz * dy : 2 * z.nkz * (dy + 1)]

        arrive(n_gz - 1, z.groups - 1)
        with jax.named_scope("last"):
            chunk_work(z, place, n_gz - 1, prm, s, x_transform)
        for which in range(2):
            copy_d(which).start()
        for part in range(2):
            for g in range(z.blocks // 2):
                x_transform(part * z.blocks // 2 + g)
            for dy in range(1, n_gy):
                copy_e(dy, part).start()

        def done(ref, sem):
            pltpu.make_async_copy(ref, ref, sem).wait()

        with jax.named_scope("drain"):
            done(cols.at[0, pl.ds(0, n_gz - 1)], send_z)
            done(cols.at[:, pl.ds(1, n_gx - 1)], send_c)
        with jax.named_scope("exchange_wait"):
            done(edges, send_d)
            done(edges, recv_d.at[0])
            done(give, send_e)
            for dy in range(1, n_gy):
                done(got.at[dy - 1], recv_e.at[dy - 1])

    pl.run_scoped(
        body,
        pltpu.VMEM((2 * z.nky, 3 * CYW), bf16),
        pltpu.VMEM((n_gz, z.cols, 3 * CZW), bf16),
        *[pltpu.VMEM((2 * z.wide, 3 * DEPTH), bf16)] * TS,
        pltpu.VMEM((z.cols, 3 * DEPTH), bf16),
        pltpu.VMEM((CX * CYW, 3 * DEPTH), bf16),
        pltpu.VMEM((3 * CZW, DEPTH), bf16),
        pltpu.VMEM((3 * CYW, DEPTH), bf16),
        pltpu.VMEM((CX * HALO, 3 * DEPTH), bf16),
    )


def add_edges(dacc, eacc):
    lane = lax.broadcasted_iota(jnp.int32, (CYW, LANES), 1)
    pad = jnp.zeros((CYW, LANES - CX * HALO), f32)
    for which, start in ((0, LANES - HALO), (1, 0)):
        e = jnp.concatenate([eacc[which], pad], axis=1)
        mask = (lane >= start) & (lane < start + HALO)
        for x in range(CX):
            v = pltpu.roll(e, (start - x * HALO) % LANES, 1)
            dacc[x] = dacc[x] + jnp.where(mask, v, 0.0)


def finish(z, own, got, dacc, edges, dens_ref, spec_ref):
    total = own[...]
    for dy in range(1, z.n_gy):
        total = total + got[dy - 1]
    spec_ref[0] = total[:, : z.nkz]
    spec_ref[1] = total[:, z.nkz :]
    dens_ref[...] = dacc[:, HALO : HALO + CY]
    dens_ref[:, CY - HALO :] = dens_ref[:, CY - HALO :] + edges[0]
    dens_ref[:, :HALO] = dens_ref[:, :HALO] + edges[1]


def x_table(z):
    idx = np.arange(z.nx)
    angle = (idx[:, None] * idx[None, :] % z.nx) * (2.0 * math.pi / z.nx)
    c, s = np.cos(angle), np.sin(angle)
    full = np.block([[c, s], [s, -c]]) / math.sqrt(z.nx * z.ny * z.nz)
    full = full.astype(np.float32)
    hi = full.astype(ml_dtypes.bfloat16)
    lo = (full - hi.astype(np.float32)).astype(ml_dtypes.bfloat16)
    return np.concatenate([hi, hi, lo], axis=1)


def shards(
    pair_blocks, basis_map, pair_cells, pair_offsets, exponent_index, radius_index, exponents
):
    n_gx, n_gy, n_gz = (lax.axis_size(a) for a in ("gx", "gy", "gz"))
    pair_dev = pair_blocks.shape[1]
    z = Sizes(n_gx, n_gy, n_gz, pair_dev)
    assert FOLD * pair_dev == LANES and n_gx % z.per == 0 and n_gz >= 3 and n_gy >= 2 and z.blocks % 2 == 0
    assert n_gx >= n_gz
    in_vmem = pl.BlockSpec(memory_space=pltpu.VMEM)
    in_hbm = pl.BlockSpec(memory_space=pltpu.HBM)
    basis = basis_map.T
    blocks = pair_blocks.T
    xt = jnp.asarray(x_table(z))
    ei, ri = exponent_index.reshape(1, -1), radius_index.reshape(1, -1)
    dma = pltpu.SemaphoreType.DMA
    own, got, dacc, edges = pl.pallas_call(
        functools.partial(kernel, z),
        out_shape=[
            jax.ShapeDtypeStruct((z.rows, 2 * z.nkz), f32),
            jax.ShapeDtypeStruct((n_gy - 1, z.rows, 2 * z.nkz), f32),
            jax.ShapeDtypeStruct((CX, CYW, CZ), f32),
            jax.ShapeDtypeStruct((2, CX, HALO, CZ), f32),
        ],
        in_specs=[in_hbm] * 8,
        out_specs=[in_vmem] * 4,
        scratch_shapes=[
            pltpu.VMEM(basis.shape, f32),
            pltpu.VMEM(blocks.shape, f32),
            pltpu.VMEM(pair_cells.shape, jnp.int32),
            pltpu.VMEM(pair_offsets.shape, f32),
            pltpu.VMEM(ei.shape, jnp.int32),
            pltpu.VMEM(ri.shape, jnp.int32),
            pltpu.SMEM(exponents.shape, f32),
            pltpu.VMEM(xt.shape, bf16),
            pltpu.VMEM((8, LANES), f32),
            pltpu.VMEM((COEFS + 8, LANES), f32),
            pltpu.VMEM((n_gz, n_gx, BLOCK_ROWS, LANES), f32),
            pltpu.VMEM((n_gy - 1, z.rows, 2 * z.nkz), f32),
            pltpu.VMEM((SIDE * SIDE, z.blocks, 2 * z.kys, LANES), f32),
            pltpu.VMEM((SIDE * SIDE, CX, LANES), f32),
            pltpu.VMEM((SIDE, CYW, LANES), f32),
            pltpu.VMEM((2, SIDE, HALO, LANES), f32),
            pltpu.VMEM((2 * z.rows, z.cols), f32),
            pltpu.VMEM((2, CYW, CX * HALO), f32),
            pltpu.SemaphoreType.REGULAR((n_gz - 1,)),
            dma((8,)),
            dma((n_gz - 1,)),
            dma((n_gz * z.groups,)),
            dma((n_gy - 1,)),
            dma((1,)),
        ],
        compiler_params=pltpu.CompilerParams(
            collective_id=0, has_side_effects=True, vmem_limit_bytes=VMEM_LIMIT
        ),
    )(
        *(
            pltpu.with_memory_space_constraint(a, pltpu.HBM)
            for a in (basis, blocks, pair_cells, pair_offsets, ei, ri, exponents, xt)
        )
    )
    dens, spec = pl.pallas_call(
        functools.partial(finish, z),
        out_shape=[
            jax.ShapeDtypeStruct((CX, CY, CZ), f32),
            jax.ShapeDtypeStruct((2, z.rows, z.nkz), f32),
        ],
        in_specs=[in_vmem] * 4,
        out_specs=[in_vmem] * 2,
        compiler_params=pltpu.CompilerParams(vmem_limit_bytes=VMEM_LIMIT),
    )(own, got, dacc, edges)
    return dens, spec.reshape(2, z.nky, z.nx, z.nkz).transpose(0, 3, 1, 2)


def solution(mesh):
    placed = (
        P(None, ("gx", "gy", "gz")),
        P(),
        P(None, ("gx", "gy", "gz")),
        P(None, ("gx", "gy", "gz")),
        P(("gx", "gy", "gz")),
        P(("gx", "gy", "gz")),
        P(),
    )
    return jax.shard_map(
        shards,
        mesh=mesh,
        in_specs=placed,
        out_specs=(P("gx", "gy", "gz"), P(None, ("gy", "gz"), "gx", None)),
        check_vma=False,
    )
```
